8 devices in a mesh: dp: 1 (over z), ep: 8 (over y, x, core).
Axes of the slice: x: 2, y: 2, z: 1, core: 2. Of those that a mesh axis runs over, the one named last changes fastest.
Arguments:
- tokens: bfloat16 [1024, 2048], P(('dp', 'ep'))
- expert_ids: int32 [1024, 8], P(('dp', 'ep'))
- norm_gain: bfloat16 [2048], replicated
- w_router: bfloat16 [2048, 64], replicated
- w_gate: bfloat16 [64, 2048, 1024], P('ep')
- w_up: bfloat16 [64, 2048, 1024], P('ep')
- w_down: bfloat16 [64, 1024, 2048], P('ep')
Outputs:
- output: bfloat16 [1024, 2048], P(('dp', 'ep'))
All inputs are finite; a program needn't handle non-finite values.
Results may differ from the reference program's by a relative error of at most 0.00578916.
Values are sent between devices in bfloat16 or wider.
A program may use at most 1 GiB of HBM per device.

```python
import jax
import jax.numpy as jnp
from jax import lax

D = 2048
EXPERTS = 64
TOP = 8
FF = 1024
TOKENS_DEV = 128
EP_SIZE = 8
BLOCK_ROWS = 128

TOKENS = EP_SIZE * TOKENS_DEV
PAIRS = TOKENS * TOP
E_LOCAL = EXPERTS // EP_SIZE
NUM_BLOCKS = PAIRS // BLOCK_ROWS + EXPERTS + 1
NORM_EPS = 1e-5


def draw_routes(route_key):
    sub_keys = jax.random.split(route_key, 6)
    pair_dev = TOKENS_DEV * TOP
    half_mean = pair_dev // (2 * EP_SIZE)
    hot_dev = jax.random.randint(sub_keys[0], (), 0, EP_SIZE)
    rotation = jax.random.randint(sub_keys[1], (), 0, EP_SIZE - 1)
    rest_weight = jax.random.randint(sub_keys[2], (EP_SIZE - 2,), 1, 3)
    rest_cum = jnp.concatenate([jnp.zeros((1,), jnp.int32), jnp.cumsum(rest_weight)])
    rest_bound = (pair_dev - 7 * half_mean) * rest_cum // rest_cum[-1]
    pattern = jnp.concatenate([jnp.full((1,), 4 * half_mean, jnp.int32), rest_bound[1:] - rest_bound[:-1]])
    src_dev = jnp.arange(EP_SIZE)[:, None]
    dst_dev = jnp.arange(EP_SIZE)[None, :]
    shift_idx = ((dst_dev - hot_dev - 1) % EP_SIZE - src_dev - rotation) % (EP_SIZE - 1)
    dev_load = jnp.where(dst_dev == hot_dev, 3 * half_mean, pattern[shift_idx])
    split_weight = jax.random.randint(sub_keys[3], (EP_SIZE, EP_SIZE, E_LOCAL), 1, 4)
    split_cum = jnp.concatenate([jnp.zeros((EP_SIZE, EP_SIZE, 1), jnp.int32), jnp.cumsum(split_weight, axis=2)], axis=2)
    split_bound = dev_load[:, :, None] * split_cum // split_cum[:, :, -1:]
    expert_count = (split_bound[:, :, 1:] - split_bound[:, :, :-1]).reshape(EP_SIZE, EXPERTS)
    count_end = jnp.cumsum(expert_count, axis=1)
    positions = jnp.arange(pair_dev)
    sorted_ids = jax.vmap(lambda end_row: jnp.searchsorted(end_row, positions, side='right'))(count_end)
    by_token = sorted_ids.reshape(EP_SIZE, TOP, TOKENS_DEV).transpose(0, 2, 1)
    tok_perm = jax.vmap(lambda perm_key: jax.random.permutation(perm_key, TOKENS_DEV))(jax.random.split(sub_keys[4], EP_SIZE))
    by_token = jnp.take_along_axis(by_token, jnp.broadcast_to(tok_perm[:, :, None], (EP_SIZE, TOKENS_DEV, TOP)), axis=1)
    turn = jax.random.randint(sub_keys[5], (EP_SIZE, TOKENS_DEV, 1), 0, TOP)
    col_idx = (jnp.arange(TOP)[None, None, :] + turn) % TOP
    by_token = jnp.take_along_axis(by_token, col_idx, axis=2)
    return by_token.reshape(TOKENS, TOP).astype(jnp.int32)


def setup_inputs(seed: int = 0, part: int = 0) -> dict:
    part_key = jax.random.fold_in(jax.random.key(seed), part)
    tok_key, route_key = jax.random.split(part_key)
    shared = jax.random.split(jax.random.key(seed + 1), 5)
    tokens = jax.random.normal(tok_key, (TOKENS, D), jnp.float32).astype(jnp.bfloat16)
    norm_gain = (1.0 + 0.3 * jax.random.normal(shared[0], (D,), jnp.float32)).astype(jnp.bfloat16)
    w_router = (jax.random.normal(shared[1], (D, EXPERTS), jnp.float32) * D ** -0.5).astype(jnp.bfloat16)
    w_gate = (jax.random.normal(shared[2], (EXPERTS, D, FF), jnp.float32) * D ** -0.5).astype(jnp.bfloat16)
    w_up = (jax.random.normal(shared[3], (EXPERTS, D, FF), jnp.float32) * D ** -0.5).astype(jnp.bfloat16)
    w_down = (jax.random.normal(shared[4], (EXPERTS, FF, D), jnp.float32) * (EXPERTS / 4 * FF ** -0.5)).astype(jnp.bfloat16)
    expert_ids = draw_routes(route_key)
    return {'tokens': tokens, 'expert_ids': expert_ids, 'norm_gain': norm_gain, 'w_router': w_router, 'w_gate': w_gate, 'w_up': w_up, 'w_down': w_down}


def reference(tokens, expert_ids, norm_gain, w_router, w_gate, w_up, w_down):
    tok32 = tokens.astype(jnp.float32)
    inv_rms = lax.rsqrt(jnp.mean(tok32 * tok32, axis=1, keepdims=True) + NORM_EPS)
    normed = (tok32 * inv_rms * norm_gain.astype(jnp.float32)).astype(jnp.bfloat16)
    logits = jnp.dot(normed, w_router, preferred_element_type=jnp.float32)
    router_prob = jax.nn.softmax(logits, axis=1)
    gate_vals = jnp.take_along_axis(router_prob, expert_ids, axis=1)
    flat_ids = expert_ids.reshape(PAIRS)
    sort_order = jnp.argsort(flat_ids, stable=True)
    sorted_ids = flat_ids[sort_order]
    counts = jnp.bincount(flat_ids, length=EXPERTS)
    padded = (counts + BLOCK_ROWS - 1) // BLOCK_ROWS * BLOCK_ROWS
    pad_end = jnp.cumsum(padded)
    group_start = jnp.cumsum(counts) - counts
    slot_sorted = pad_end[sorted_ids] - padded[sorted_ids] + jnp.arange(PAIRS) - group_start[sorted_ids]
    row_buf = jnp.zeros((NUM_BLOCKS * BLOCK_ROWS, D), jnp.bfloat16).at[slot_sorted].set(normed[sort_order // TOP])
    block_expert = jnp.minimum(jnp.searchsorted(pad_end, jnp.arange(NUM_BLOCKS) * BLOCK_ROWS, side='right'), EXPERTS - 1)

    def block_apply(block_args):
        block_rows, expert = block_args
        hidden_gate = jnp.dot(block_rows, w_gate[expert], preferred_element_type=jnp.float32)
        hidden_up = jnp.dot(block_rows, w_up[expert], preferred_element_type=jnp.float32)
        swiglu_out = (jax.nn.silu(hidden_gate) * hidden_up).astype(jnp.bfloat16)
        return jnp.dot(swiglu_out, w_down[expert], preferred_element_type=jnp.float32).astype(jnp.bfloat16)

    block_out = lax.map(block_apply, (row_buf.reshape(NUM_BLOCKS, BLOCK_ROWS, D), block_expert))
    slot_pair = jnp.zeros((PAIRS,), jnp.int32).at[sort_order].set(slot_sorted)
    pair_out = block_out.reshape(NUM_BLOCKS * BLOCK_ROWS, D)[slot_pair].reshape(TOKENS, TOP, D)
    moe_sum = jnp.einsum('nk,nkd->nd', gate_vals, pair_out.astype(jnp.float32))
    return (tok32 + moe_sum).astype(jnp.bfloat16)
```

```python
import functools

import jax
import jax.numpy as jnp
from jax import lax
from jax.experimental import pallas as pl
from jax.experimental.pallas import tpu as pltpu
from jax.sharding import PartitionSpec as P

NORM_EPS = 1e-5
MESH = pl.DeviceIdType.MESH
F32, BF16, I32 = jnp.float32, jnp.bfloat16, jnp.int32
FC = 128
CC = 256
WIN = 256
RG = 16


def moe_kernel(dims, x_ref, ids_ref, gain_ref, wr_ref, w1_ref, w3_ref, w2_ref, out_ref,
               xg, idsg, ug, gbuf, xs, hbuf, pbuf, gates, wa, wb, obuf, part, rd, rp1, rp2,
               meta_v, meta_s, posrow,
               s_ids, r_ids, s_own, s_fwd, r_sib, r_x, r_y, r_dg, r_sf, s_w, s_meta,
               d_s, d_r, p1_s, p1_r, p2_s, p2_r):
    T, D, FF, E, NDEV, NB = dims
    NF, NC = FF // FC, D // CC
    HT = T // 2
    me = lax.axis_index('ep')
    core = me % 2
    cx = (me // 2) % 2
    cy = me // 4
    sib = cy * 4 + cx * 2 + (1 - core)
    xn = cy * 4 + (1 - cx) * 2 + core
    yn = (1 - cy) * 4 + cx * 2 + core
    dg = (1 - cy) * 4 + (1 - cx) * 2 + core

    def remote(src, dst, ss, rs, dev):
        return pltpu.make_async_remote_copy(src_ref=src, dst_ref=dst, send_sem=ss, recv_sem=rs,
                                            device_id={'ep': dev}, device_id_type=MESH)

    wslots = (wa, wb)

    def a_copies(f, slot):
        cols = pl.ds(pl.multiple_of(f * FC, FC), FC)
        return (pltpu.make_async_copy(w1_ref.at[:, :, cols], wslots[slot].at[:, :, pl.ds(0, FC)], s_w.at[slot, 0]),
                pltpu.make_async_copy(w3_ref.at[:, :, cols], wslots[slot].at[:, :, pl.ds(FC, FC)], s_w.at[slot, 1]))

    def b_copy(c, slot, half):
        cols = pl.ds(pl.multiple_of(c * CC, CC), CC)
        rows = pl.ds(pl.multiple_of(half * FF, FF), FF)
        return pltpu.make_async_copy(w2_ref.at[:, :, cols], wslots[slot].at[:, rows, :], s_w.at[slot, half])

    for slot in range(2):
        for cp in a_copies(slot, slot):
            cp.start()

    barrier = pltpu.get_barrier_semaphore()
    for k in range(1, NDEV):
        pl.semaphore_signal(barrier, inc=1, device_id={'ep': (me + k) % NDEV}, device_id_type=MESH)
    pl.semaphore_wait(barrier, NDEV - 1)

    def ids_copy(k):
        return remote(ids_ref, idsg.at[me], s_ids.at[k - 1], r_ids.at[k - 1], (me + k) % NDEV)

    for k in range(1, NDEV):
        ids_copy(k).start()
    own_sib = remote(x_ref, xg.at[me], s_own.at[0], r_sib, sib)
    h0, h1 = pl.ds(0, HT), pl.ds(HT, HT)
    halves = (h0, h1)

    def own_x(h):
        return remote(x_ref.at[halves[h], :], xg.at[me, halves[h], :], s_own.at[1 + h], r_x.at[h], xn)

    def own_y(h):
        return remote(x_ref.at[halves[h], :], xg.at[me, halves[h], :], s_own.at[3 + h], r_y.at[h], yn)

    own_x(0).start()
    own_y(1).start()
    own_x(1).start()
    own_y(0).start()
    own_sib.start()

    def norm_rows(src, row0):
        def body(i, carry):
            rows = pl.ds(pl.multiple_of(i * 16, 16), 16)
            t = src[rows, :].astype(F32)
            inv = lax.rsqrt(jnp.mean(t * t, axis=1, keepdims=True) + NORM_EPS)
            ug[pl.ds(pl.multiple_of(row0 + i * 16, 16), 16), :] = (t * inv * gain_ref[...].astype(F32)).astype(BF16)
            return carry
        lax.fori_loop(0, T // 16, body, 0)

    norm_rows(x_ref, core * T)

    idsg[me] = ids_ref[...]
    for k in range(1, NDEV):
        ids_copy(k).wait_recv()
    sub_e = lax.broadcasted_iota(I32, (E, T), 0)
    lane = lax.broadcasted_iota(I32, (E, T), 1)
    masks = []
    for s in range(NDEV):
        ids = idsg[s]
        m = jnp.zeros((E, T), I32)
        for j in range(ids.shape[0]):
            m = m + (ids[j:j + 1, :] == sub_e + me * E).astype(I32)
        masks.append(m)
    tri = (lax.broadcasted_iota(I32, (T, T), 0) <= lax.broadcasted_iota(I32, (T, T), 1)).astype(F32).astype(BF16)
    counts = [jnp.sum(m, axis=1, keepdims=True) for m in masks]
    total = counts[0]
    for s in range(1, NDEV):
        total = total + counts[s]
    nblk = (total + (T - 1)) // T
    nblk = jnp.broadcast_to(nblk, (E, T))
    start = jnp.zeros((E, T), I32)
    for e in range(E - 1):
        start = start + jnp.where(sub_e > e, jnp.broadcast_to(nblk[e:e + 1, :], (E, T)), 0)
    eid = jnp.sum((start + nblk <= lane).astype(I32), axis=0, keepdims=True)
    eid = jnp.minimum(eid, E - 1)
    base = start * T
    wst = jnp.zeros((E, T), I32)
    poss = []
    for s in range(NDEV):
        rank = jnp.dot(masks[s].astype(F32).astype(BF16), tri, preferred_element_type=F32).astype(I32)
        pos = jnp.where(masks[s] > 0, base + rank - 1, -1)
        poss.append(pos)
        for e in range(E):
            posrow[e, s] = jnp.broadcast_to(pos[e:e + 1, :], (8, T))
        w0 = jnp.minimum(base // RG, (NB * T - WIN) // RG)
        wst = wst + jnp.where(lane == s, w0, 0)
        base = base + counts[s]
    meta_v[0:E, :] = wst
    meta_v[E:2 * E, :] = jnp.broadcast_to(eid, (E, T))
    meta_copy = pltpu.make_async_copy(meta_v, meta_s, s_meta)
    meta_copy.start()
    meta_copy.wait()
    wlane = lax.broadcasted_iota(I32, (T, WIN), 1)
    for s in range(NDEV):
        padded = jnp.concatenate([poss[s], jnp.zeros((T - E, T), I32)], axis=0).astype(F32)
        col = padded.T
        for e in range(E):
            pc = col[:, e:e + 1].astype(I32)
            pbuf[s, e] = (pc == wlane + meta_s[e, s] * RG).astype(F32).astype(BF16)

    def route_chip(chip, first):
        logits = jnp.dot(ug[...], wr_ref[...], preferred_element_type=F32)
        both = jnp.concatenate([logits, logits], axis=1)
        ex = jnp.exp(both - jnp.max(both, axis=1, keepdims=True))
        prob = ex / (jnp.sum(ex, axis=1, keepdims=True) * 0.5)
        prob = pltpu.roll(prob, (128 - me * E) % 128, 1)
        gates[chip * 2] = prob[:T]
        gates[chip * 2 + 1] = prob[T:]

        def build(b, carry):
            e = meta_s[E, b]
            rows = lax.broadcasted_iota(I32, (T, T), 0) + b * T
            for c in range(2):
                p = jnp.broadcast_to(posrow[e, chip * 2 + c][0:1, :], (T, T))
                gbuf[pl.ds(pl.multiple_of(b * T, T), T), c * T:(c + 1) * T] = (p == rows).astype(F32).astype(BF16)
            return carry
        lax.fori_loop(0, NB, build, 0)
        MR = NB * T // 4

        def gather(i, carry):
            rows = pl.ds(pl.multiple_of((i // 4) * MR, 16), MR)
            cols = pl.ds(pl.multiple_of((i % 4) * (D // 4), 128), D // 4)
            got = jnp.dot(gbuf[rows, :], ug[:, cols], preferred_element_type=F32).astype(BF16)
            if first:
                xs[rows, cols] = got
            else:
                xs[rows, cols] = xs[rows, cols] + got
            return carry
        lax.fori_loop(0, 16, gather, 0)

    def sib_fwd(kind, h, src_dev):
        return remote(xg.at[src_dev, halves[h], :], xg.at[src_dev, halves[h], :],
                      s_fwd.at[2 + kind * 2 + h], r_sf.at[kind, h], sib)

    own_sib.wait_recv()
    norm_rows(xg.at[sib], (1 - core) * T)
    route_chip(cy * 2 + cx, True)

    own_x(0).wait_recv()
    fwd_y = remote(xg.at[xn, h0, :], xg.at[xn, h0, :], s_fwd.at[0], r_dg.at[0], yn)
    fwd_y.start()
    sib_fwd(0, 0, xn).start()
    own_y(1).wait_recv()
    fwd_x = remote(xg.at[yn, h1, :], xg.at[yn, h1, :], s_fwd.at[1], r_dg.at[1], xn)
    fwd_x.start()
    sib_fwd(1, 1, yn).start()
    own_x(1).wait_recv()
    sib_fwd(0, 1, xn).start()
    own_y(0).wait_recv()
    sib_fwd(1, 0, yn).start()

    def take(kind, dev, chip):
        norm_rows(xg.at[dev], core * T)
        other = dev + 1 - 2 * core
        for h in range(2):
            sib_fwd(kind, h, dev).wait_recv()
        norm_rows(xg.at[other], (1 - core) * T)
        route_chip(chip, False)

    take(0, xn, cy * 2 + (1 - cx))
    take(1, yn, (1 - cy) * 2 + cx)
    fwd_y.wait_recv()
    sib_fwd(2, 0, dg).start()
    fwd_x.wait_recv()
    sib_fwd(2, 1, dg).start()
    take(2, dg, (1 - cy) * 2 + (1 - cx))

    def hidden(g, carry):
        for slot in range(2):
            f = g * 2 + slot
            for cp in a_copies(f, slot):
                cp.wait()
            cols = pl.ds(pl.multiple_of(f * FC, FC), FC)
            for b in range(NB):
                e = meta_s[E, b]
                acc = jnp.dot(xs[b * T:(b + 1) * T, :], wslots[slot][e], preferred_element_type=F32)
                hg, hu = acc[:, :FC], acc[:, FC:]
                hbuf[b * T:(b + 1) * T, cols] = (jax.nn.silu(hg) * hu).astype(BF16)

            @pl.when(g < NF // 2 - 1)
            def _():
                for cp in a_copies(f + 2, slot):
                    cp.start()

            @pl.when(g >= NF // 2 - 1)
            def _():
                for h in range(2):
                    b_copy(slot * 2 + h, slot, h).start()
        return carry

    lax.fori_loop(0, NF // 2, hidden, 0)

    def d2d(j):
        return remote(part.at[j % 4, 1 - core], rd.at[j], d_s.at[j], d_r.at[j], sib)

    def first_hop(j):
        return (remote(part.at[j % 4, core, 0, :, 1 - cx], rp1.at[j, 0], p1_s.at[j, 0], p1_r.at[j, 0], xn),
                remote(part.at[j % 4, core, 1, 1 - cy], rp1.at[j, 1], p1_s.at[j, 1], p1_r.at[j, 1], yn))

    def second_hop(j):
        return (remote(part.at[j % 4, core, 0, 1 - cy, cx], rp2.at[j, 0], p2_s.at[j, 0], p2_r.at[j, 0], yn),
                remote(part.at[j % 4, core, 1, cy, 1 - cx], rp2.at[j, 1], p2_s.at[j, 1], p2_r.at[j, 1], xn))

    def combine(c, to_core):
        for ch in range(NDEV // 2):
            s = ch * 2 + to_core
            acc = jnp.zeros((T, CC), F32)
            for e in range(E):
                r0 = meta_s[e, s]
                rows = jnp.concatenate([obuf[r0 + k] for k in range(WIN // RG)], axis=0)
                got = jnp.dot(pbuf[s, e], rows, preferred_element_type=F32)
                acc = acc + gates[s, :, e:e + 1] * got
            for h in range(2):
                part[c % 4, to_core, h, ch // 2, ch % 2] = acc[:, h * 128:(h + 1) * 128]

    def outputs(i, half, slot):
        rows = pl.ds(pl.multiple_of(half * FF, FF), FF)
        for b in range(NB):
            e = meta_s[E, b]
            acc = jnp.dot(hbuf[b * T:(b + 1) * T, :], wslots[slot][e, rows, :], preferred_element_type=F32)
            obuf[b * (T // RG):(b + 1) * (T // RG)] = acc.astype(BF16).reshape(T // RG, RG, CC)
        combine(i, 1 - core)
        d2d(i).start()
        combine(i, core)

    def drain(i):
        @pl.when((i >= 1) & (i < NC + 1))
        def _():
            j = i - 1
            d2d(j).wait_recv()
            for h in range(2):
                for ch in range(NDEV // 2):
                    at = (j % 4, core, h, ch // 2, ch % 2)
                    part[at] = part[at] + rd[j, h, ch // 2, ch % 2]
            for cp in first_hop(j):
                cp.start()

        @pl.when((i >= 2) & (i < NC + 2))
        def _():
            j = i - 2
            for h, cp in enumerate(first_hop(j)):
                cp.wait_recv()
                for k in range(2):
                    at = (j % 4, core, h, k, cx) if h == 0 else (j % 4, core, h, cy, k)
                    part[at] = part[at] + rp1[j, h, k]
            for cp in second_hop(j):
                cp.start()

        @pl.when(i >= 3)
        def _():
            j = i - 3
            for h, cp in enumerate(second_hop(j)):
                cp.wait_recv()
                cols = pl.ds(pl.multiple_of(j * CC + h * 128, 128), 128)
                moe = part[j % 4, core, h, cy, cx] + rp2[j, h]
                out_ref[:, cols] = (x_ref[:, cols].astype(F32) + moe).astype(BF16)
            d2d(j).wait_send()
            for cp in first_hop(j):
                cp.wait_send()
            for cp in second_hop(j):
                cp.wait_send()

    def four(g, carry):
        for slot in range(2):
            for h in range(2):
                b_copy(g * 4 + slot * 2 + h, slot, h).wait()

            def two(half, inner):
                i = g * 4 + slot * 2 + half
                outputs(i, half, slot)
                drain(i)
                return inner
            lax.fori_loop(0, 2, two, 0)

            @pl.when(g < NC // 4 - 1)
            def _():
                for h in range(2):
                    b_copy((g + 1) * 4 + slot * 2 + h, slot, h).start()
        return carry

    lax.fori_loop(0, NC // 4, four, 0)

    def last(i, carry):
        drain(i)
        return carry

    lax.fori_loop(NC, NC + 3, last, 0)

    for k in range(1, NDEV):
        ids_copy(k).wait_send()
    own_sib.wait_send()
    for h in range(2):
        own_x(h).wait_send()
        own_y(h).wait_send()
    fwd_y.wait_send()
    fwd_x.wait_send()
    for kind, dev in enumerate((xn, yn, dg)):
        for h in range(2):
            sib_fwd(kind, h, dev).wait_send()


def solution(mesh):
    ndev = mesh.shape['ep']

    def device_step(tokens, expert_ids, norm_gain, w_router, w_gate, w_up, w_down):
        T, D = tokens.shape
        top = expert_ids.shape[1]
        E, _, FF = w_gate.shape
        NR = w_router.shape[1]
        most = 3 * T * top // 2
        NB = (most + E * (T - 1)) // T
        NC = D // CC
        dims = (T, D, FF, E, ndev, NB)
        vmem = pl.BlockSpec(memory_space=pltpu.VMEM)
        hbm = pl.BlockSpec(memory_space=pl.ANY)
        dma = pltpu.SemaphoreType.DMA
        return pl.pallas_call(
            functools.partial(moe_kernel, dims),
            out_shape=jax.ShapeDtypeStruct((T, D), BF16),
            in_specs=[vmem, vmem, vmem, vmem, hbm, hbm, hbm],
            out_specs=vmem,
            scratch_shapes=[
                pltpu.VMEM((ndev, T, D), BF16),
                pltpu.VMEM((ndev, top, T), I32),
                pltpu.VMEM((2 * T, D), BF16),
                pltpu.VMEM((NB * T, 2 * T), BF16),
                pltpu.VMEM((NB * T, D), BF16),
                pltpu.VMEM((NB * T, FF), BF16),
                pltpu.VMEM((ndev, E, T, WIN), BF16),
                pltpu.VMEM((ndev, T, 128), F32),
                pltpu.VMEM((E, D, 2 * FC), BF16),
                pltpu.VMEM((E, D, 2 * FC), BF16),
                pltpu.VMEM((NB * T // RG, RG, CC), BF16),
                pltpu.VMEM((4, 2, 2, 2, 2, T, 128), F32),
                pltpu.VMEM((NC, 2, 2, 2, T, 128), F32),
                pltpu.VMEM((NC, 2, 2, T, 128), F32),
                pltpu.VMEM((NC, 2, T, 128), F32),
                pltpu.VMEM((2 * E, T), I32),
                pltpu.SMEM((2 * E, T), I32),
                pltpu.VMEM((E, ndev, 8, T), I32),
                dma((ndev - 1,)), dma((ndev - 1,)),
                dma((5,)), dma((8,)),
                dma, dma((2,)), dma((2,)), dma((2,)), dma((3, 2)),
                dma((2, 2)), dma,
                dma((NC,)), dma((NC,)), dma((NC, 2)), dma((NC, 2)), dma((NC, 2)), dma((NC, 2)),
            ],
            compiler_params=pltpu.CompilerParams(
                collective_id=0, has_side_effects=True, vmem_limit_bytes=67043328),
            name='moe_block',
        )(tokens, expert_ids.T, norm_gain.reshape(1, D), w_router, w_gate, w_up, w_down)

    row_spec = P(('dp', 'ep'), None)
    expert_spec = P('ep', None, None)
    return jax.shard_map(device_step, mesh=mesh,
                         in_specs=(row_spec, row_spec, P(None), P(None, None), expert_spec, expert_spec, expert_spec),
                         out_specs=row_spec, check_vma=False)
```

```python
import functools

import jax
import jax.numpy as jnp
from jax import lax
from jax.experimental import pallas as pl
from jax.experimental.pallas import tpu as pltpu
from jax.sharding import PartitionSpec as P

NORM_EPS = 1e-5
MESH = pl.DeviceIdType.MESH
F32, BF16, I32 = jnp.float32, jnp.bfloat16, jnp.int32
FC = 128
CC = 256
NQ = 4
WIN = 256
RG = 16


def moe_kernel(dims, x_ref, ids_ref, gain_ref, wr_ref, w1_ref, w3_ref, w2_ref, out_ref,
               xg, idsg, gsrc, gdst, gbuf, xs, hbuf, pbuf, gates, wa, wb, obuf, part, rd, rp1, rp2,
               meta_v, meta_s, posrow,
               s_ids, r_ids, s_gt, r_gt, s_sib, r_sib, s_nb, r_nb, s_dg, r_dg, s_sf, r_sf, s_sd, r_sd, s_w, s_meta,
               d_s, d_r, p1_s, p1_r, p2_s, p2_r):
    T, D, FF, E, NDEV, NB = dims
    NF, NC = FF // FC, D // CC
    HT = T // 2
    me = lax.axis_index('ep')
    core = me % 2
    cx = (me // 2) % 2
    cy = me // 4
    sib = cy * 4 + cx * 2 + (1 - core)
    xn = cy * 4 + (1 - cx) * 2 + core
    yn = (1 - cy) * 4 + cx * 2 + core

    def remote(src, dst, ss, rs, dev):
        return pltpu.make_async_remote_copy(src_ref=src, dst_ref=dst, send_sem=ss, recv_sem=rs,
                                            device_id={'ep': dev}, device_id_type=MESH)

    wslots = (wa, wb)

    def a_copies(f, slot):
        cols = pl.ds(pl.multiple_of(f * FC, FC), FC)
        return (pltpu.make_async_copy(w1_ref.at[:, :, cols], wslots[slot].at[:, :, pl.ds(0, FC)], s_w.at[slot, 0]),
                pltpu.make_async_copy(w3_ref.at[:, :, cols], wslots[slot].at[:, :, pl.ds(FC, FC)], s_w.at[slot, 1]))

    def b_copy(c, slot, half):
        cols = pl.ds(pl.multiple_of(c * CC, CC), CC)
        rows = pl.ds(pl.multiple_of(half * FF, FF), FF)
        return pltpu.make_async_copy(w2_ref.at[:, :, cols], wslots[slot].at[:, rows, :], s_w.at[slot, half])

    for slot in range(2):
        for cp in a_copies(slot, slot):
            cp.start()

    barrier = pltpu.get_barrier_semaphore()
    for k in range(1, NDEV):
        pl.semaphore_signal(barrier, inc=1, device_id={'ep': (me + k) % NDEV}, device_id_type=MESH)

    own = xg.at[me // 2, core]

    def norm_rows(i, carry):
        rows = pl.ds(pl.multiple_of(i * 16, 16), 16)
        t = x_ref[rows, :].astype(F32)
        inv = lax.rsqrt(jnp.mean(t * t, axis=1, keepdims=True) + NORM_EPS)
        xg[me // 2, core, rows, :] = (t * inv * gain_ref[...].astype(F32).reshape(1, D)).astype(BF16)
        return carry

    lax.fori_loop(0, T // 16, norm_rows, 0)
    pl.semaphore_wait(barrier, NDEV - 1)

    def ids_copy(k):
        return remote(ids_ref, idsg.at[me], s_ids.at[k - 1], r_ids.at[k - 1], (me + k) % NDEV)

    def gate_copy(k):
        to = (me + k) % NDEV
        return remote(gsrc.at[to], gdst.at[me], s_gt.at[k - 1], r_gt.at[k - 1], to)

    chip_x = cy * 2 + (1 - cx)
    chip_y = (1 - cy) * 2 + cx
    chip_d = (1 - cy) * 2 + (1 - cx)
    chip_me = cy * 2 + cx
    QC = D // NQ

    def part_of(chip, q, rows=pl.ds(0, T)):
        return xg.at[chip, core, rows, pl.ds(q * QC, QC)]

    def to_sib(q):
        return remote(part_of(chip_me, q), part_of(chip_me, q), s_sib.at[q], r_sib.at[q], sib)

    def to_nb(k, q):
        return remote(part_of(chip_me, q), part_of(chip_me, q), s_nb.at[k, q], r_nb.at[k, q], (xn, yn)[k])

    halves = (pl.ds(0, HT), pl.ds(HT, HT))

    def to_diag(k, q):
        src = part_of((chip_x, chip_y)[k], q, halves[k])
        return remote(src, src, s_dg.at[k, q], r_dg.at[k, q], (yn, xn)[k])

    def nb_sib(k, q):
        src = part_of((chip_x, chip_y)[k], q)
        return remote(src, src, s_sf.at[k, q], r_sf.at[k, q], sib)

    def diag_sib(k, q):
        src = part_of(chip_d, q, halves[k])
        return remote(src, src, s_sd.at[k, q], r_sd.at[k, q], sib)

    for k in range(1, NDEV):
        ids_copy(k).start()
    for q in range(NQ):
        to_nb(0, q).start()
        to_nb(1, q).start()
        to_sib(q).start()

    logits = lax.dot_general(wr_ref[...], own[...], (((1,), (1,)), ((), ())), preferred_element_type=F32)
    ex = jnp.exp(logits - jnp.max(logits, axis=0, keepdims=True))
    prob = ex / jnp.sum(ex, axis=0, keepdims=True)
    for r in range(NDEV):
        gsrc[r] = prob[r * E:(r + 1) * E]
    gdst[me] = gsrc[me]

    idsg[me] = ids_ref[...]
    for k in range(1, NDEV):
        ids_copy(k).wait_recv()
    sub_e = lax.broadcasted_iota(I32, (E, T), 0)
    lane = lax.broadcasted_iota(I32, (E, T), 1)
    masks = []
    for s in range(NDEV):
        ids = idsg[s]
        m = jnp.zeros((E, T), I32)
        for j in range(ids.shape[0]):
            m = m + (ids[j:j + 1, :] == sub_e + me * E).astype(I32)
        masks.append(m)
    tri = (lax.broadcasted_iota(I32, (T, T), 0) <= lax.broadcasted_iota(I32, (T, T), 1)).astype(F32).astype(BF16)
    counts = [jnp.sum(m, axis=1, keepdims=True) for m in masks]
    total = counts[0]
    for s in range(1, NDEV):
        total = total + counts[s]
    nblk = (total + (T - 1)) // T
    nblk = jnp.broadcast_to(nblk, (E, T))
    start = jnp.zeros((E, T), I32)
    for e in range(E - 1):
        start = start + jnp.where(sub_e > e, jnp.broadcast_to(nblk[e:e + 1, :], (E, T)), 0)
    eid = jnp.sum((start + nblk <= lane).astype(I32), axis=0, keepdims=True)
    eid = jnp.minimum(eid, E - 1)
    base = start * T
    wst = jnp.zeros((E, T), I32)
    poss = []
    for s in range(NDEV):
        rank = jnp.dot(masks[s].astype(F32).astype(BF16), tri, preferred_element_type=F32).astype(I32)
        pos = jnp.where(masks[s] > 0, base + rank - 1, -1)
        poss.append(pos)
        for e in range(E):
            posrow[e, s] = jnp.broadcast_to(pos[e:e + 1, :], (8, T))
        w0 = jnp.minimum(base // RG, (NB * T - WIN) // RG)
        wst = wst + jnp.where(lane == s, w0, 0)
        base = base + counts[s]
    meta_v[0:E, :] = wst
    meta_v[E:2 * E, :] = jnp.broadcast_to(eid, (E, T))
    meta_copy = pltpu.make_async_copy(meta_v, meta_s, s_meta)
    meta_copy.start()
    meta_copy.wait()
    for k in range(1, NDEV):
        gate_copy(k).start()

    def build(b, carry):
        e = meta_s[E, b]
        rows = lax.broadcasted_iota(I32, (T, T), 0) + b * T
        for s in range(NDEV):
            p = jnp.broadcast_to(posrow[e, s][0:1, :], (T, T))
            gbuf[s // 2, pl.ds(pl.multiple_of(b * T, T), T), (s % 2) * T:(s % 2 + 1) * T] = (p == rows).astype(F32).astype(BF16)
        return carry

    lax.fori_loop(0, NB, build, 0)
    MR = NB * T // 4

    def gather(q, chips, add):
        cols = pl.ds(q * QC, QC)

        def body(i, carry):
            rows = pl.ds(pl.multiple_of(i * MR, 16), MR)
            got = None
            for chip in chips:
                one = jnp.dot(gbuf[chip, rows, :], xg[chip, :, :, cols].reshape(2 * T, QC), preferred_element_type=F32)
                got = one if got is None else got + one
            got = got.astype(BF16)
            xs[rows, cols] = xs[rows, cols] + got if add else got
            return carry
        lax.fori_loop(0, 4, body, 0)

    for q in range(NQ):
        for k in range(2):
            to_nb(k, q).wait_recv()
            to_diag(k, q).start()
            nb_sib(k, q).start()
        if q > 0:
            gather(q - 1, (chip_me, chip_x, chip_y), False)
        to_sib(q).wait_recv()
        for k in range(2):
            nb_sib(k, q).wait_recv()
    gather(NQ - 1, (chip_me, chip_x, chip_y), False)

    wlane = lax.broadcasted_iota(I32, (T, WIN), 1)

    def windows(s):
        padded = jnp.concatenate([poss[s], jnp.zeros((T - E, T), I32)], axis=0).astype(F32)
        col = padded.T
        for e in range(E):
            pc = col[:, e:e + 1].astype(I32)
            pbuf[s, e] = (pc == wlane + meta_s[e, s] * RG).astype(F32).astype(BF16)
        gates[s] = jnp.concatenate([gdst[s], jnp.zeros((T - E, T), F32)], axis=0).T

    for k in range(1, NDEV):
        gate_copy(k).wait_recv()
    for q in range(NQ):
        for k in range(2):
            to_diag(k, q).wait_recv()
            diag_sib(k, q).start()
        windows(2 * q)
        windows(2 * q + 1)
        for k in range(2):
            diag_sib(k, q).wait_recv()
        gather(q, (chip_d,), True)

    def hidden(g, carry):
        for slot in range(2):
            f = g * 2 + slot
            for cp in a_copies(f, slot):
                cp.wait()
            cols = pl.ds(pl.multiple_of(f * FC, FC), FC)
            for b in range(NB):
                e = meta_s[E, b]
                acc = jnp.dot(xs[b * T:(b + 1) * T, :], wslots[slot][e], preferred_element_type=F32)
                hg, hu = acc[:, :FC], acc[:, FC:]
                hbuf[b * T:(b + 1) * T, cols] = (jax.nn.silu(hg) * hu).astype(BF16)

            @pl.when(g < NF // 2 - 1)
            def _():
                for cp in a_copies(f + 2, slot):
                    cp.start()

            @pl.when(g >= NF // 2 - 1)
            def _():
                for h in range(2):
                    b_copy(slot * 2 + h, slot, h).start()
        return carry

    lax.fori_loop(0, NF // 2, hidden, 0)

    def d2d(j):
        return remote(part.at[j % 4, 1 - core], rd.at[j], d_s.at[j], d_r.at[j], sib)

    def first_hop(j):
        return (remote(part.at[j % 4, core, 0, :, 1 - cx], rp1.at[j, 0], p1_s.at[j, 0], p1_r.at[j, 0], xn),
                remote(part.at[j % 4, core, 1, 1 - cy], rp1.at[j, 1], p1_s.at[j, 1], p1_r.at[j, 1], yn))

    def second_hop(j):
        return (remote(part.at[j % 4, core, 0, 1 - cy, cx], rp2.at[j, 0], p2_s.at[j, 0], p2_r.at[j, 0], yn),
                remote(part.at[j % 4, core, 1, cy, 1 - cx], rp2.at[j, 1], p2_s.at[j, 1], p2_r.at[j, 1], xn))

    def combine(c, to_core):
        for ch in range(NDEV // 2):
            s = ch * 2 + to_core
            acc = jnp.zeros((T, CC), F32)
            for e in range(E):
                r0 = meta_s[e, s]
                rows = jnp.concatenate([obuf[r0 + k] for k in range(WIN // RG)], axis=0)
                got = jnp.dot(pbuf[s, e], rows, preferred_element_type=F32)
                acc = acc + gates[s, :, e:e + 1] * got
            for h in range(2):
                part[c % 4, to_core, h, ch // 2, ch % 2] = acc[:, h * 128:(h + 1) * 128]

    def outputs(i, half, slot):
        rows = pl.ds(pl.multiple_of(half * FF, FF), FF)
        for b in range(NB):
            e = meta_s[E, b]
            acc = jnp.dot(hbuf[b * T:(b + 1) * T, :], wslots[slot][e, rows, :], preferred_element_type=F32)
            obuf[b * (T // RG):(b + 1) * (T // RG)] = acc.astype(BF16).reshape(T // RG, RG, CC)
        combine(i, 1 - core)
        d2d(i).start()
        combine(i, core)

    def drain(i):
        @pl.when((i >= 1) & (i < NC + 1))
        def _():
            j = i - 1
            d2d(j).wait_recv()
            for h in range(2):
                for ch in range(NDEV // 2):
                    at = (j % 4, core, h, ch // 2, ch % 2)
                    part[at] = part[at] + rd[j, h, ch // 2, ch % 2]
            for cp in first_hop(j):
                cp.start()

        @pl.when((i >= 2) & (i < NC + 2))
        def _():
            j = i - 2
            for h, cp in enumerate(first_hop(j)):
                cp.wait_recv()
                for k in range(2):
                    at = (j % 4, core, h, k, cx) if h == 0 else (j % 4, core, h, cy, k)
                    part[at] = part[at] + rp1[j, h, k]
            for cp in second_hop(j):
                cp.start()

        @pl.when(i >= 3)
        def _():
            j = i - 3
            for h, cp in enumerate(second_hop(j)):
                cp.wait_recv()
                cols = pl.ds(pl.multiple_of(j * CC + h * 128, 128), 128)
                moe = part[j % 4, core, h, cy, cx] + rp2[j, h]
                out_ref[:, cols] = (x_ref[:, cols].astype(F32) + moe).astype(BF16)
            d2d(j).wait_send()
            for cp in first_hop(j):
                cp.wait_send()
            for cp in second_hop(j):
                cp.wait_send()

    def four(g, carry):
        for slot in range(2):
            for h in range(2):
                b_copy(g * 4 + slot * 2 + h, slot, h).wait()

            def two(half, inner):
                i = g * 4 + slot * 2 + half
                outputs(i, half, slot)
                drain(i)
                return inner
            lax.fori_loop(0, 2, two, 0)

            @pl.when(g < NC // 4 - 1)
            def _():
                for h in range(2):
                    b_copy((g + 1) * 4 + slot * 2 + h, slot, h).start()
        return carry

    lax.fori_loop(0, NC // 4, four, 0)

    def last(i, carry):
        drain(i)
        return carry

    lax.fori_loop(NC, NC + 3, last, 0)

    for k in range(1, NDEV):
        ids_copy(k).wait_send()
        gate_copy(k).wait_send()
    for q in range(NQ):
        to_sib(q).wait_send()
        for k in range(2):
            for move in (to_nb, to_diag, nb_sib, diag_sib):
                move(k, q).wait_send()


def solution(mesh):
    ndev = mesh.shape['ep']

    def device_step(tokens, expert_ids, norm_gain, w_router, w_gate, w_up, w_down):
        T, D = tokens.shape
        top = expert_ids.shape[1]
        E, _, FF = w_gate.shape
        most = 3 * T * top // 2
        NB = (most + E * (T - 1)) // T
        NC = D // CC
        dims = (T, D, FF, E, ndev, NB)
        vmem = pl.BlockSpec(memory_space=pltpu.VMEM)
        hbm = pl.BlockSpec(memory_space=pl.ANY)
        dma = pltpu.SemaphoreType.DMA
        return pl.pallas_call(
            functools.partial(moe_kernel, dims),
            out_shape=jax.ShapeDtypeStruct((T, D), BF16),
            in_specs=[vmem, vmem, vmem, vmem, hbm, hbm, hbm],
            out_specs=vmem,
            scratch_shapes=[
                pltpu.VMEM((ndev // 2, 2, T, D), BF16),
                pltpu.VMEM((ndev, top, T), I32),
                pltpu.VMEM((ndev, E, T), F32),
                pltpu.VMEM((ndev, E, T), F32),
                pltpu.VMEM((ndev // 2, NB * T, 2 * T), BF16),
                pltpu.VMEM((NB * T, D), BF16),
                pltpu.VMEM((NB * T, FF), BF16),
                pltpu.VMEM((ndev, E, T, WIN), BF16),
                pltpu.VMEM((ndev, T, 128), F32),
                pltpu.VMEM((E, D, 2 * FC), BF16),
                pltpu.VMEM((E, D, 2 * FC), BF16),
                pltpu.VMEM((NB * T // RG, RG, CC), BF16),
                pltpu.VMEM((4, 2, 2, 2, 2, T, 128), F32),
                pltpu.VMEM((NC, 2, 2, 2, T, 128), F32),
                pltpu.VMEM((NC, 2, 2, T, 128), F32),
                pltpu.VMEM((NC, 2, T, 128), F32),
                pltpu.VMEM((2 * E, T), I32),
                pltpu.SMEM((2 * E, T), I32),
                pltpu.VMEM((E, ndev, 8, T), I32),
                dma((ndev - 1,)), dma((ndev - 1,)),
                dma((ndev - 1,)), dma((ndev - 1,)),
                dma((NQ,)), dma((NQ,)), dma((2, NQ)), dma((2, NQ)),
                dma((2, NQ)), dma((2, NQ)), dma((2, NQ)), dma((2, NQ)), dma((2, NQ)), dma((2, NQ)),
                dma((2, 2)), dma,
                dma((NC,)), dma((NC,)), dma((NC, 2)), dma((NC, 2)), dma((NC, 2)), dma((NC, 2)),
            ],
            compiler_params=pltpu.CompilerParams(
                collective_id=0, has_side_effects=True, vmem_limit_bytes=67043328),
            name='moe_block',
        )(tokens, expert_ids.T, norm_gain, w_router.T, w_gate, w_up, w_down)

    row_spec = P(('dp', 'ep'), None)
    expert_spec = P('ep', None, None)
    return jax.shard_map(device_step, mesh=mesh,
                         in_specs=(row_spec, row_spec, P(None), P(None, None), expert_spec, expert_spec, expert_spec),
                         out_specs=row_spec, check_vma=False)
```

```python
import functools

import jax
import jax.numpy as jnp
from jax import lax
from jax.experimental import pallas as pl
from jax.experimental.pallas import tpu as pltpu
from jax.sharding import PartitionSpec as P

NORM_EPS = 1e-5
MESH = pl.DeviceIdType.MESH
F32, BF16, I32 = jnp.float32, jnp.bfloat16, jnp.int32
FC = 128
CC = 256
NSLOT = 3
NQ = 4
WIN = 256
RG = 16


def moe_kernel(dims, x_hbm, ids_hbm, gain_hbm, wr_hbm, w1_ref, w3_ref, w2_ref, out_ref,
               x_ref, gain_ref, wr_ref, xg, idsg, gsrc, gdst, gbuf, xs, hbuf, gates, wa, wb, wc, obuf, part, rd, rp1, rp2,
               meta_v, meta_s, posrow, posv, s_in,
               s_ids, r_ids, s_gt, r_gt, s_sib, r_sib, s_nb, r_nb, s_dg, r_dg, s_sf, r_sf, s_sd, r_sd, s_w, s_meta,
               d_s, d_r, p1_s, p1_r, p2_s, p2_r):
    T, D, FF, E, NDEV, NB = dims
    NF, NC = FF // FC, D // CC
    HT = T // 2
    me = lax.axis_index('ep')
    core = me % 2
    cx = (me // 2) % 2
    cy = me // 4
    sib = cy * 4 + cx * 2 + (1 - core)
    xn = cy * 4 + (1 - cx) * 2 + core
    yn = (1 - cy) * 4 + cx * 2 + core

    def remote(src, dst, ss, rs, dev):
        return pltpu.make_async_remote_copy(src_ref=src, dst_ref=dst, send_sem=ss, recv_sem=rs,
                                            device_id={'ep': dev}, device_id_type=MESH)

    wslots = (wa, wb, wc)

    def a_copies(f, slot):
        cols = pl.ds(pl.multiple_of(f * FC, FC), FC)
        return (pltpu.make_async_copy(w1_ref.at[:, :, cols], wslots[slot].at[:, :, pl.ds(0, FC)], s_w.at[slot, 0]),
                pltpu.make_async_copy(w3_ref.at[:, :, cols], wslots[slot].at[:, :, pl.ds(FC, FC)], s_w.at[slot, 1]))

    def b_copy(c, slot, half):
        cols = pl.ds(pl.multiple_of(c * CC, CC), CC)
        rows = pl.ds(pl.multiple_of(half * FF, FF), FF)
        return pltpu.make_async_copy(w2_ref.at[:, :, cols], wslots[slot].at[:, rows, :], s_w.at[slot, half])

    barrier = pltpu.get_barrier_semaphore()
    for k in range(1, NDEV):
        pl.semaphore_signal(barrier, inc=1, device_id={'ep': (me + k) % NDEV}, device_id_type=MESH)

    ins = [pltpu.make_async_copy(a, b, s_in.at[k]) for k, (a, b) in enumerate(
        ((x_hbm, x_ref), (gain_hbm, gain_ref), (ids_hbm, idsg.at[me]), (wr_hbm, wr_ref)))]
    for cp in ins:
        cp.start()
    for slot in range(NSLOT):
        for cp in a_copies(slot, slot):
            cp.start()

    own = xg.at[me // 2, core]

    ins[0].wait()
    ins[1].wait()
    gain = gain_ref[...].astype(F32).reshape(1, D)
    for i in range(T // 16):
        rows = pl.ds(i * 16, 16)
        t = x_ref[rows, :].astype(F32)
        inv = lax.rsqrt(jnp.mean(t * t, axis=1, keepdims=True) + NORM_EPS)
        xg[me // 2, core, rows, :] = (t * inv * gain).astype(BF16)
    ins[2].wait()
    pl.semaphore_wait(barrier, NDEV - 1)

    def ids_copy(k):
        return remote(idsg.at[me], idsg.at[me], s_ids.at[k - 1], r_ids.at[k - 1], (me + k) % NDEV)

    def gate_copy(k):
        to = (me + k) % NDEV
        return remote(gsrc.at[to], gdst.at[me], s_gt.at[k - 1], r_gt.at[k - 1], to)

    chip_x = cy * 2 + (1 - cx)
    chip_y = (1 - cy) * 2 + cx
    chip_d = (1 - cy) * 2 + (1 - cx)
    chip_me = cy * 2 + cx
    QC = D // NQ

    def part_of(chip, q, rows=pl.ds(0, T)):
        return xg.at[chip, core, rows, pl.ds(q * QC, QC)]

    def to_sib(q):
        return remote(part_of(chip_me, q), part_of(chip_me, q), s_sib.at[q], r_sib.at[q], sib)

    def to_nb(k, q):
        return remote(part_of(chip_me, q), part_of(chip_me, q), s_nb.at[k, q], r_nb.at[k, q], (xn, yn)[k])

    halves = (pl.ds(0, HT), pl.ds(HT, HT))

    def to_diag(k, q):
        src = part_of((chip_x, chip_y)[k], q, halves[k])
        return remote(src, src, s_dg.at[k, q], r_dg.at[k, q], (yn, xn)[k])

    def nb_sib(k, q):
        src = part_of((chip_x, chip_y)[k], q)
        return remote(src, src, s_sf.at[k, q], r_sf.at[k, q], sib)

    def diag_sib(k, q):
        src = part_of(chip_d, q, halves[k])
        return remote(src, src, s_sd.at[k, q], r_sd.at[k, q], sib)

    for k in range(1, NDEV):
        ids_copy(k).start()
    for q in range(NQ):
        to_nb(0, q).start()
        to_nb(1, q).start()
        to_sib(q).start()

    ins[3].wait()
    logits = lax.dot_general(wr_ref[...], own[...], (((1,), (1,)), ((), ())), preferred_element_type=F32)
    ex = jnp.exp(logits - jnp.max(logits, axis=0, keepdims=True))
    prob = ex / jnp.sum(ex, axis=0, keepdims=True)
    for r in range(NDEV):
        gsrc[r] = prob[r * E:(r + 1) * E]
    gdst[me] = gsrc[me]

    for k in range(1, NDEV):
        ids_copy(k).wait_recv()
    sub_e = lax.broadcasted_iota(I32, (E, T), 0)
    lane = lax.broadcasted_iota(I32, (E, T), 1)
    masks = []
    for s in range(NDEV):
        ids = idsg[s]
        m = jnp.zeros((E, T), I32)
        for j in range(ids.shape[0]):
            m = m + (ids[j:j + 1, :] == sub_e + me * E).astype(I32)
        masks.append(m)
    tri = (lax.broadcasted_iota(I32, (T, T), 0) <= lax.broadcasted_iota(I32, (T, T), 1)).astype(F32).astype(BF16)
    counts = [jnp.sum(m, axis=1, keepdims=True) for m in masks]
    total = counts[0]
    for s in range(1, NDEV):
        total = total + counts[s]
    nblk = (total + (T - 1)) // T
    nblk = jnp.broadcast_to(nblk, (E, T))
    start = jnp.zeros((E, T), I32)
    for e in range(E - 1):
        start = start + jnp.where(sub_e > e, jnp.broadcast_to(nblk[e:e + 1, :], (E, T)), 0)
    eid = jnp.sum((start + nblk <= lane).astype(I32), axis=0, keepdims=True)
    eid = jnp.minimum(eid, E - 1)
    base = start * T
    wst = jnp.zeros((E, T), I32)
    for s in range(NDEV):
        rank = jnp.dot(masks[s].astype(F32).astype(BF16), tri, preferred_element_type=F32).astype(I32)
        pos = jnp.where(masks[s] > 0, base + rank - 1, -1)
        posv[s] = pos
        for e in range(E):
            posrow[e, s] = jnp.broadcast_to(pos[e:e + 1, :], (8, T))
        w0 = jnp.minimum(base // RG, (NB * T - WIN) // RG)
        wst = wst + jnp.where(lane == s, w0, 0)
        base = base + counts[s]
    meta_v[0:E, :] = wst
    meta_v[E:2 * E, :] = jnp.broadcast_to(eid, (E, T))
    meta_copy = pltpu.make_async_copy(meta_v, meta_s, s_meta)
    meta_copy.start()
    meta_copy.wait()
    for k in range(1, NDEV):
        gate_copy(k).start()

    def build(b, carry):
        e = meta_s[E, b]
        rows = lax.broadcasted_iota(I32, (T, T), 0) + b * T
        for s in range(NDEV):
            p = jnp.broadcast_to(posrow[e, s][0:1, :], (T, T))
            gbuf[s // 2, pl.ds(pl.multiple_of(b * T, T), T), (s % 2) * T:(s % 2 + 1) * T] = (p == rows).astype(F32).astype(BF16)
        return carry

    lax.fori_loop(0, NB, build, 0)
    MR = NB * T // 4

    def gather(q, chips, add):
        cols = pl.ds(q * QC, QC)

        def body(i, carry):
            rows = pl.ds(pl.multiple_of(i * MR, 16), MR)
            got = None
            for chip in chips:
                one = jnp.dot(gbuf[chip, rows, :], xg[chip, :, :, cols].reshape(2 * T, QC), preferred_element_type=F32)
                got = one if got is None else got + one
            got = got.astype(BF16)
            xs[rows, cols] = xs[rows, cols] + got if add else got
            return carry
        lax.fori_loop(0, 4, body, 0)

    for q in range(NQ):
        for k in range(2):
            to_nb(k, q).wait_recv()
            to_diag(k, q).start()
            nb_sib(k, q).start()
        if q > 0:
            gather(q - 1, (chip_me, chip_x, chip_y), False)
        to_sib(q).wait_recv()
        for k in range(2):
            nb_sib(k, q).wait_recv()
    gather(NQ - 1, (chip_me, chip_x, chip_y), False)

    for k in range(1, NDEV):
        gate_copy(k).wait_recv()
    for q in range(NQ):
        for k in range(2):
            to_diag(k, q).wait_recv()
            diag_sib(k, q).start()
        for k in range(2):
            diag_sib(k, q).wait_recv()
        gather(q, (chip_d,), True)

    wlane = lax.broadcasted_iota(I32, (T, WIN), 1)

    def window_rows(s, e):
        return pl.ds(pl.multiple_of((s % 2 * E + e) * T, T), T)

    def windows(s):
        padded = jnp.concatenate([posv[s], jnp.zeros((T - E, T), I32)], axis=0).astype(F32)
        col = padded.T
        for e in range(E):
            pc = col[:, e:e + 1].astype(I32)
            gbuf[s // 2, window_rows(s, e), :] = (pc == wlane + meta_s[e, s] * RG).astype(F32).astype(BF16)
        gates[s] = jnp.concatenate([gdst[s], jnp.zeros((T - E, T), F32)], axis=0).T

    def hidden(f, slot):
        for cp in a_copies(f, slot):
            cp.wait()
        windows(f)
        cols = pl.ds(pl.multiple_of(f * FC, FC), FC)
        for b in range(NB):
            e = meta_s[E, b]
            acc = jnp.dot(xs[b * T:(b + 1) * T, :], wslots[slot][e], preferred_element_type=F32)
            hg, hu = acc[:, :FC], acc[:, FC:]
            hbuf[b * T:(b + 1) * T, cols] = (jax.nn.silu(hg) * hu).astype(BF16)

    def hidden_three(g, carry):
        for slot in range(NSLOT):
            f = g * NSLOT + slot
            hidden(f, slot)

            @pl.when(f < NF - NSLOT)
            def _():
                for cp in a_copies(f + NSLOT, slot):
                    cp.start()
        return carry

    lax.fori_loop(0, NF // NSLOT, hidden_three, 0)
    order = (2, 0)
    for h in range(2):
        b_copy(h, order[0], h).start()
    hidden(NF - 2, 0)
    for h in range(2):
        b_copy(2 + h, order[1], h).start()
    hidden(NF - 1, 1)

    def d2d(j):
        return remote(part.at[j % 4, 1 - core], rd.at[j], d_s.at[j], d_r.at[j], sib)

    def first_hop(j):
        return (remote(part.at[j % 4, core, 0, :, 1 - cx], rp1.at[j, 0], p1_s.at[j, 0], p1_r.at[j, 0], xn),
                remote(part.at[j % 4, core, 1, 1 - cy], rp1.at[j, 1], p1_s.at[j, 1], p1_r.at[j, 1], yn))

    def second_hop(j):
        return (remote(part.at[j % 4, core, 0, 1 - cy, cx], rp2.at[j, 0], p2_s.at[j, 0], p2_r.at[j, 0], yn),
                remote(part.at[j % 4, core, 1, cy, 1 - cx], rp2.at[j, 1], p2_s.at[j, 1], p2_r.at[j, 1], xn))

    def combine(c, to_core):
        for ch in range(NDEV // 2):
            s = ch * 2 + to_core
            acc = jnp.zeros((T, CC), F32)
            for e in range(E):
                r0 = meta_s[e, s]
                rows = jnp.concatenate([obuf[r0 + k] for k in range(WIN // RG)], axis=0)
                got = jnp.dot(gbuf[s // 2, window_rows(s, e), :], rows, preferred_element_type=F32)
                acc = acc + gates[s, :, e:e + 1] * got
            for h in range(2):
                part[c % 4, to_core, h, ch // 2, ch % 2] = acc[:, h * 128:(h + 1) * 128]

    def outputs(half, slot):
        rows = pl.ds(pl.multiple_of(half * FF, FF), FF)
        for b in range(NB):
            e = meta_s[E, b]
            acc = jnp.dot(hbuf[b * T:(b + 1) * T, :], wslots[slot][e, rows, :], preferred_element_type=F32)
            obuf[b * (T // RG):(b + 1) * (T // RG)] = acc.astype(BF16).reshape(T // RG, RG, CC)

    def drain(i):
        @pl.when((i >= 1) & (i < NC + 1))
        def _():
            j = i - 1
            d2d(j).wait_recv()
            for h in range(2):
                for ch in range(NDEV // 2):
                    at = (j % 4, core, h, ch // 2, ch % 2)
                    part[at] = part[at] + rd[j, h, ch // 2, ch % 2]
            for cp in first_hop(j):
                cp.start()

        @pl.when((i >= 2) & (i < NC + 2))
        def _():
            j = i - 2
            for h, cp in enumerate(first_hop(j)):
                cp.wait_recv()
                for k in range(2):
                    at = (j % 4, core, h, k, cx) if h == 0 else (j % 4, core, h, cy, k)
                    part[at] = part[at] + rp1[j, h, k]
            for cp in second_hop(j):
                cp.start()

        @pl.when(i >= 3)
        def _():
            j = i - 3
            for h, cp in enumerate(second_hop(j)):
                cp.wait_recv()
                cols = pl.ds(pl.multiple_of(j * CC + h * 128, 128), 128)
                moe = part[j % 4, core, h, cy, cx] + rp2[j, h]
                out_ref[:, cols] = (x_ref[:, cols].astype(F32) + moe).astype(BF16)
            d2d(j).wait_send()
            for cp in first_hop(j):
                cp.wait_send()
            for cp in second_hop(j):
                cp.wait_send()

    def four(g, carry):
        for t in range(2):
            slot = order[t]
            for h in range(2):
                b_copy(g * 4 + t * 2 + h, slot, h).wait()

            def two(half, inner):
                i = g * 4 + t * 2 + half
                outputs(half, slot)
                drain(i)
                combine(i, 1 - core)
                d2d(i).start()
                combine(i, core)
                return inner
            lax.fori_loop(0, 2, two, 0)

            @pl.when(g < NC // 4 - 1)
            def _():
                for h in range(2):
                    b_copy((g + 1) * 4 + t * 2 + h, slot, h).start()
        return carry

    lax.fori_loop(0, NC // 4, four, 0)

    def last(i, carry):
        drain(i)
        return carry

    lax.fori_loop(NC, NC + 3, last, 0)

    for k in range(1, NDEV):
        ids_copy(k).wait_send()
        gate_copy(k).wait_send()
    for q in range(NQ):
        to_sib(q).wait_send()
        for k in range(2):
            for move in (to_nb, to_diag, nb_sib, diag_sib):
                move(k, q).wait_send()


def solution(mesh):
    ndev = mesh.shape['ep']

    def device_step(tokens, expert_ids, norm_gain, w_router, w_gate, w_up, w_down):
        T, D = tokens.shape
        top = expert_ids.shape[1]
        E, _, FF = w_gate.shape
        most = 3 * T * top // 2
        NB = (most + E * (T - 1)) // T
        NC = D // CC
        dims = (T, D, FF, E, ndev, NB)
        vmem = pl.BlockSpec(memory_space=pltpu.VMEM)
        hbm = pl.BlockSpec(memory_space=pl.ANY)
        dma = pltpu.SemaphoreType.DMA
        return pl.pallas_call(
            functools.partial(moe_kernel, dims),
            out_shape=jax.ShapeDtypeStruct((T, D), BF16),
            in_specs=[hbm] * 7,
            out_specs=vmem,
            scratch_shapes=[
                pltpu.VMEM((T, D), BF16),
                pltpu.VMEM((D,), BF16),
                pltpu.VMEM((ndev * E, D), BF16),
                pltpu.VMEM((ndev // 2, 2, T, D), BF16),
                pltpu.VMEM((ndev, top, T), I32),
                pltpu.VMEM((ndev, E, T), F32),
                pltpu.VMEM((ndev, E, T), F32),
                pltpu.VMEM((ndev // 2, NB * T, 2 * T), BF16),
                pltpu.VMEM((NB * T, D), BF16),
                pltpu.VMEM((NB * T, FF), BF16),
                pltpu.VMEM((ndev, T, 128), F32),
                pltpu.VMEM((E, D, 2 * FC), BF16),
                pltpu.VMEM((E, D, 2 * FC), BF16),
                pltpu.VMEM((E, D, 2 * FC), BF16),
                pltpu.VMEM((NB * T // RG, RG, CC), BF16),
                pltpu.VMEM((4, 2, 2, 2, 2, T, 128), F32),
                pltpu.VMEM((NC, 2, 2, 2, T, 128), F32),
                pltpu.VMEM((NC, 2, 2, T, 128), F32),
                pltpu.VMEM((NC, 2, T, 128), F32),
                pltpu.VMEM((2 * E, T), I32),
                pltpu.SMEM((2 * E, T), I32),
                pltpu.VMEM((E, ndev, 8, T), I32),
                pltpu.VMEM((ndev, E, T), I32),
                dma((4,)),
                dma((ndev - 1,)), dma((ndev - 1,)),
                dma((ndev - 1,)), dma((ndev - 1,)),
                dma((NQ,)), dma((NQ,)), dma((2, NQ)), dma((2, NQ)),
                dma((2, NQ)), dma((2, NQ)), dma((2, NQ)), dma((2, NQ)), dma((2, NQ)), dma((2, NQ)),
                dma((NSLOT, 2)), dma,
                dma((NC,)), dma((NC,)), dma((NC, 2)), dma((NC, 2)), dma((NC, 2)), dma((NC, 2)),
            ],
            compiler_params=pltpu.CompilerParams(
                collective_id=0, has_side_effects=True, vmem_limit_bytes=67043328),
            name='moe_block',
        )(tokens, expert_ids.T, norm_gain, w_router.T, w_gate, w_up, w_down)

    row_spec = P(('dp', 'ep'), None)
    expert_spec = P('ep', None, None)
    return jax.shard_map(device_step, mesh=mesh,
                         in_specs=(row_spec, row_spec, P(None), P(None, None), expert_spec, expert_spec, expert_spec),
                         out_specs=row_spec, check_vma=False)
```

```python
import functools

import jax
import jax.numpy as jnp
from jax import lax
from jax.experimental import pallas as pl
from jax.experimental.pallas import tpu as pltpu
from jax.sharding import PartitionSpec as P

NORM_EPS = 1e-5
MESH = pl.DeviceIdType.MESH
F32, BF16, I32 = jnp.float32, jnp.bfloat16, jnp.int32
FC = 128
CC = 256
NSLOT = 3
NQ = 4
WIN = 256
RG = 16


def moe_kernel(dims, x_hbm, ids_hbm, gain_hbm, wr_hbm, w1_ref, w3_ref, w2_ref, out_ref,
               x_ref, gain_ref, wr_ref, xg, idsg, gsrc, gdst, gbuf, xs, hbuf, gates, wa, wb, wc, obuf, part, rd, rp1, rp2,
               meta_v, meta_s, posrow, posv, s_in,
               s_ids, r_ids, s_gt, r_gt, s_sib, r_sib, s_nb, r_nb, s_dg, r_dg, s_sf, r_sf, s_sd, r_sd, s_w, s_meta,
               d_s, d_r, p1_s, p1_r, p2_s, p2_r):
    T, D, FF, E, NDEV, NB = dims
    NF, NC = FF // FC, D // CC
    HT = T // 2
    me = lax.axis_index('ep')
    core = me % 2
    cx = (me // 2) % 2
    cy = me // 4
    sib = cy * 4 + cx * 2 + (1 - core)
    xn = cy * 4 + (1 - cx) * 2 + core
    yn = (1 - cy) * 4 + cx * 2 + core

    def remote(src, dst, ss, rs, dev):
        return pltpu.make_async_remote_copy(src_ref=src, dst_ref=dst, send_sem=ss, recv_sem=rs,
                                            device_id={'ep': dev}, device_id_type=MESH)

    wslots = (wa, wb, wc)

    def a_copies(f, slot):
        cols = pl.ds(pl.multiple_of(f * FC, FC), FC)
        return (pltpu.make_async_copy(w1_ref.at[:, :, cols], wslots[slot].at[:, :, pl.ds(0, FC)], s_w.at[slot, 0]),
                pltpu.make_async_copy(w3_ref.at[:, :, cols], wslots[slot].at[:, :, pl.ds(FC, FC)], s_w.at[slot, 1]))

    def b_copy(c, slot, half):
        cols = pl.ds(pl.multiple_of(c * CC, CC), CC)
        rows = pl.ds(pl.multiple_of(half * FF, FF), FF)
        return pltpu.make_async_copy(w2_ref.at[:, :, cols], wslots[slot].at[:, rows, :], s_w.at[slot, half])

    barrier = pltpu.get_barrier_semaphore()
    for k in range(1, NDEV):
        pl.semaphore_signal(barrier, inc=1, device_id={'ep': (me + k) % NDEV}, device_id_type=MESH)

    ins = [pltpu.make_async_copy(a, b, s_in.at[k]) for k, (a, b) in enumerate(
        ((x_hbm, x_ref), (gain_hbm, gain_ref), (ids_hbm, idsg.at[me]), (wr_hbm, wr_ref)))]
    for cp in ins:
        cp.start()
    for slot in range(NSLOT):
        for cp in a_copies(slot, slot):
            cp.start()

    own = xg.at[me // 2, core]

    ins[0].wait()
    ins[1].wait()
    gain = gain_ref[...].astype(F32).reshape(1, D)
    for i in range(T // 16):
        rows = pl.ds(i * 16, 16)
        t = x_ref[rows, :].astype(F32)
        inv = lax.rsqrt(jnp.mean(t * t, axis=1, keepdims=True) + NORM_EPS)
        xg[me // 2, core, rows, :] = (t * inv * gain).astype(BF16)
    ins[2].wait()
    pl.semaphore_wait(barrier, NDEV - 1)

    def ids_copy(k):
        return remote(idsg.at[me], idsg.at[me], s_ids.at[k - 1], r_ids.at[k - 1], (me + k) % NDEV)

    def gate_copy(k):
        to = (me + k) % NDEV
        return remote(gsrc.at[to], gdst.at[me], s_gt.at[k - 1], r_gt.at[k - 1], to)

    chip_x = cy * 2 + (1 - cx)
    chip_y = (1 - cy) * 2 + cx
    chip_d = (1 - cy) * 2 + (1 - cx)
    chip_me = cy * 2 + cx
    QC = D // NQ

    def part_of(chip, q, rows=pl.ds(0, T)):
        return xg.at[chip, core, rows, pl.ds(pl.multiple_of(q * QC, QC), QC)]

    def to_sib(q):
        return remote(part_of(chip_me, q), part_of(chip_me, q), s_sib.at[q], r_sib.at[q], sib)

    def to_nb(k, q):
        return remote(part_of(chip_me, q), part_of(chip_me, q), s_nb.at[k, q], r_nb.at[k, q], (xn, yn)[k])

    halves = (pl.ds(0, HT), pl.ds(HT, HT))

    def to_diag(k, q):
        src = part_of((chip_x, chip_y)[k], q, halves[k])
        return remote(src, src, s_dg.at[k, q], r_dg.at[k, q], (yn, xn)[k])

    def nb_sib(k, q):
        src = part_of((chip_x, chip_y)[k], q)
        return remote(src, src, s_sf.at[k, q], r_sf.at[k, q], sib)

    def diag_sib(k, q):
        src = part_of(chip_d, q, halves[k])
        return remote(src, src, s_sd.at[k, q], r_sd.at[k, q], sib)

    for k in range(1, NDEV):
        ids_copy(k).start()
    for q in range(NQ):
        to_nb(0, q).start()
        to_nb(1, q).start()
        to_sib(q).start()

    ins[3].wait()
    logits = lax.dot_general(wr_ref[...], own[...], (((1,), (1,)), ((), ())), preferred_element_type=F32)
    ex = jnp.exp(logits - jnp.max(logits, axis=0, keepdims=True))
    prob = ex / jnp.sum(ex, axis=0, keepdims=True)
    for r in range(NDEV):
        gsrc[r] = prob[r * E:(r + 1) * E]
    gdst[me] = gsrc[me]

    for k in range(1, NDEV):
        ids_copy(k).wait_recv()
    sub_e = lax.broadcasted_iota(I32, (E, T), 0)
    lane = lax.broadcasted_iota(I32, (E, T), 1)
    masks = []
    for s in range(NDEV):
        ids = idsg[s]
        m = jnp.zeros((E, T), I32)
        for j in range(ids.shape[0]):
            m = m + (ids[j:j + 1, :] == sub_e + me * E).astype(I32)
        masks.append(m)
    tri = (lax.broadcasted_iota(I32, (T, T), 0) <= lax.broadcasted_iota(I32, (T, T), 1)).astype(F32).astype(BF16)
    counts = [jnp.sum(m, axis=1, keepdims=True) for m in masks]
    total = counts[0]
    for s in range(1, NDEV):
        total = total + counts[s]
    nblk = (total + (T - 1)) // T
    nblk = jnp.broadcast_to(nblk, (E, T))
    start = jnp.zeros((E, T), I32)
    for e in range(E - 1):
        start = start + jnp.where(sub_e > e, jnp.broadcast_to(nblk[e:e + 1, :], (E, T)), 0)
    eid = jnp.sum((start + nblk <= lane).astype(I32), axis=0, keepdims=True)
    eid = jnp.minimum(eid, E - 1)
    base = start * T
    wst = jnp.zeros((E, T), I32)
    for s in range(NDEV):
        rank = jnp.dot(masks[s].astype(F32).astype(BF16), tri, preferred_element_type=F32).astype(I32)
        pos = jnp.where(masks[s] > 0, base + rank - 1, -1)
        posv[s] = pos
        for e in range(E):
            posrow[e, s] = jnp.broadcast_to(pos[e:e + 1, :], (8, T))
        w0 = jnp.minimum(base // RG, (NB * T - WIN) // RG)
        wst = wst + jnp.where(lane == s, w0, 0)
        base = base + counts[s]
    meta_v[0:E, :] = wst
    meta_v[E:2 * E, :] = jnp.broadcast_to(eid, (E, T))
    meta_copy = pltpu.make_async_copy(meta_v, meta_s, s_meta)
    meta_copy.start()
    meta_copy.wait()
    for k in range(1, NDEV):
        gate_copy(k).start()

    def build(b, carry):
        e = meta_s[E, b]
        rows = lax.broadcasted_iota(I32, (T, T), 0) + b * T
        for s in range(NDEV):
            p = jnp.broadcast_to(posrow[e, s][0:1, :], (T, T))
            gbuf[s // 2, pl.ds(pl.multiple_of(b * T, T), T), (s % 2) * T:(s % 2 + 1) * T] = (p == rows).astype(F32).astype(BF16)
        return carry

    lax.fori_loop(0, NB, build, 0)
    MR = NB * T // 4

    def gather(q, chips, add):
        cols = pl.ds(pl.multiple_of(q * QC, QC), QC)
        for i in range(4):
            rows = pl.ds(i * MR, MR)
            got = None
            for chip in chips:
                one = jnp.dot(gbuf[chip, rows, :], xg[chip, :, :, cols].reshape(2 * T, QC), preferred_element_type=F32)
                got = one if got is None else got + one
            got = got.astype(BF16)
            xs[rows, cols] = xs[rows, cols] + got if add else got

    def forward(q):
        for k in range(2):
            to_nb(k, q).wait_recv()
            to_diag(k, q).start()
            nb_sib(k, q).start()

    def gather_near(q):
        to_sib(q).wait_recv()
        for k in range(2):
            nb_sib(k, q).wait_recv()
        gather(q, (chip_me, chip_x, chip_y), False)

    def forward_diag(q):
        for k in range(2):
            to_diag(k, q).wait_recv()
            diag_sib(k, q).start()

    forward(0)

    def near(q, carry):
        @pl.when(q < NQ - 1)
        def _():
            forward(q + 1)

        @pl.when(q == NQ - 1)
        def _():
            forward_diag(0)
        gather_near(q)
        return carry

    lax.fori_loop(0, NQ, near, 0)

    def far(q, carry):
        @pl.when(q < NQ - 1)
        def _():
            forward_diag(q + 1)
        for k in range(2):
            diag_sib(k, q).wait_recv()
        gather(q, (chip_d,), True)
        return carry

    lax.fori_loop(0, NQ, far, 0)
    for k in range(1, NDEV):
        gate_copy(k).wait_recv()

    wlane = lax.broadcasted_iota(I32, (T, WIN), 1)

    def window_rows(s, e):
        return pl.ds(pl.multiple_of((s % 2 * E + e) * T, T), T)

    def windows(s):
        padded = jnp.concatenate([posv[s], jnp.zeros((T - E, T), I32)], axis=0).astype(F32)
        col = padded.T
        for e in range(E):
            pc = col[:, e:e + 1].astype(I32)
            gbuf[s // 2, window_rows(s, e), :] = (pc == wlane + meta_s[e, s] * RG).astype(F32).astype(BF16)
        gates[s] = jnp.concatenate([gdst[s], jnp.zeros((T - E, T), F32)], axis=0).T

    def hidden(f, slot):
        for cp in a_copies(f, slot):
            cp.wait()
        windows(f)
        cols = pl.ds(pl.multiple_of(f * FC, FC), FC)
        for b in range(NB):
            e = meta_s[E, b]
            acc = jnp.dot(xs[b * T:(b + 1) * T, :], wslots[slot][e], preferred_element_type=F32)
            hg, hu = acc[:, :FC], acc[:, FC:]
            hbuf[b * T:(b + 1) * T, cols] = (jax.nn.silu(hg) * hu).astype(BF16)

    order = (2, 0)

    def hidden_three(g, carry):
        for slot in range(NSLOT):
            f = g * NSLOT + slot

            @pl.when(f < NF)
            def _():
                hidden(f, slot)

            @pl.when(f < NF - NSLOT)
            def _():
                for cp in a_copies(f + NSLOT, slot):
                    cp.start()

            if slot in order:
                @pl.when((f >= NF - NSLOT) & (f < NF))
                def _():
                    for h in range(2):
                        b_copy(order.index(slot) * 2 + h, slot, h).start()
        return carry

    lax.fori_loop(0, (NF + NSLOT - 1) // NSLOT, hidden_three, 0)

    def d2d(j):
        return remote(part.at[j % 4, 1 - core], rd.at[j], d_s.at[j], d_r.at[j], sib)

    def first_hop(j):
        return (remote(part.at[j % 4, core, 0, :, 1 - cx], rp1.at[j, 0], p1_s.at[j, 0], p1_r.at[j, 0], xn),
                remote(part.at[j % 4, core, 1, 1 - cy], rp1.at[j, 1], p1_s.at[j, 1], p1_r.at[j, 1], yn))

    def second_hop(j):
        return (remote(part.at[j % 4, core, 0, 1 - cy, cx], rp2.at[j, 0], p2_s.at[j, 0], p2_r.at[j, 0], yn),
                remote(part.at[j % 4, core, 1, cy, 1 - cx], rp2.at[j, 1], p2_s.at[j, 1], p2_r.at[j, 1], xn))

    def combine(c, to_core):
        for ch in range(NDEV // 2):
            s = ch * 2 + to_core
            acc = jnp.zeros((T, CC), F32)
            for e in range(E):
                r0 = meta_s[e, s]
                rows = jnp.concatenate([obuf[r0 + k] for k in range(WIN // RG)], axis=0)
                got = jnp.dot(gbuf[s // 2, window_rows(s, e), :], rows, preferred_element_type=F32)
                acc = acc + gates[s, :, e:e + 1] * got
            for h in range(2):
                part[c % 4, to_core, h, ch // 2, ch % 2] = acc[:, h * 128:(h + 1) * 128]

    def outputs(half, slot):
        rows = pl.ds(pl.multiple_of(half * FF, FF), FF)
        for b in range(NB):
            e = meta_s[E, b]
            acc = jnp.dot(hbuf[b * T:(b + 1) * T, :], wslots[slot][e, rows, :], preferred_element_type=F32)
            obuf[b * (T // RG):(b + 1) * (T // RG)] = acc.astype(BF16).reshape(T // RG, RG, CC)

    def drain(i):
        @pl.when((i >= 1) & (i < NC + 1))
        def _():
            j = i - 1
            d2d(j).wait_recv()
            for h in range(2):
                for ch in range(NDEV // 2):
                    at = (j % 4, core, h, ch // 2, ch % 2)
                    part[at] = part[at] + rd[j, h, ch // 2, ch % 2]
            for cp in first_hop(j):
                cp.start()

        @pl.when((i >= 2) & (i < NC + 2))
        def _():
            j = i - 2
            for h, cp in enumerate(first_hop(j)):
                cp.wait_recv()
                for k in range(2):
                    at = (j % 4, core, h, k, cx) if h == 0 else (j % 4, core, h, cy, k)
                    part[at] = part[at] + rp1[j, h, k]
            for cp in second_hop(j):
                cp.start()

        @pl.when(i >= 3)
        def _():
            j = i - 3
            for h, cp in enumerate(second_hop(j)):
                cp.wait_recv()
                cols = pl.ds(pl.multiple_of(j * CC + h * 128, 128), 128)
                moe = part[j % 4, core, h, cy, cx] + rp2[j, h]
                out_ref[:, cols] = (x_ref[:, cols].astype(F32) + moe).astype(BF16)
            d2d(j).wait_send()
            for cp in first_hop(j):
                cp.wait_send()
            for cp in second_hop(j):
                cp.wait_send()

    def four(g, carry):
        for t in range(2):
            slot = order[t]
            for h in range(2):
                b_copy(g * 4 + t * 2 + h, slot, h).wait()

            def two(half, inner):
                i = g * 4 + t * 2 + half
                outputs(half, slot)
                drain(i)
                combine(i, 1 - core)
                d2d(i).start()
                combine(i, core)
                return inner
            lax.fori_loop(0, 2, two, 0)

            @pl.when(g < NC // 4 - 1)
            def _():
                for h in range(2):
                    b_copy((g + 1) * 4 + t * 2 + h, slot, h).start()
        return carry

    lax.fori_loop(0, NC // 4, four, 0)

    def last(i, carry):
        drain(i)
        return carry

    lax.fori_loop(NC, NC + 3, last, 0)

    for k in range(1, NDEV):
        ids_copy(k).wait_send()
        gate_copy(k).wait_send()
    for q in range(NQ):
        to_sib(q).wait_send()
        for k in range(2):
            for move in (to_nb, to_diag, nb_sib, diag_sib):
                move(k, q).wait_send()


def solution(mesh):
    ndev = mesh.shape['ep']

    def device_step(tokens, expert_ids, norm_gain, w_router, w_gate, w_up, w_down):
        T, D = tokens.shape
        top = expert_ids.shape[1]
        E, _, FF = w_gate.shape
        most = 3 * T * top // 2
        NB = (most + E * (T - 1)) // T
        NC = D // CC
        dims = (T, D, FF, E, ndev, NB)
        vmem = pl.BlockSpec(memory_space=pltpu.VMEM)
        hbm = pl.BlockSpec(memory_space=pl.ANY)
        dma = pltpu.SemaphoreType.DMA
        return pl.pallas_call(
            functools.partial(moe_kernel, dims),
            out_shape=jax.ShapeDtypeStruct((T, D), BF16),
            in_specs=[hbm] * 7,
            out_specs=vmem,
            scratch_shapes=[
                pltpu.VMEM((T, D), BF16),
                pltpu.VMEM((D,), BF16),
                pltpu.VMEM((ndev * E, D), BF16),
                pltpu.VMEM((ndev // 2, 2, T, D), BF16),
                pltpu.VMEM((ndev, top, T), I32),
                pltpu.VMEM((ndev, E, T), F32),
                pltpu.VMEM((ndev, E, T), F32),
                pltpu.VMEM((ndev // 2, NB * T, 2 * T), BF16),
                pltpu.VMEM((NB * T, D), BF16),
                pltpu.VMEM((NB * T, FF), BF16),
                pltpu.VMEM((ndev, T, 128), F32),
                pltpu.VMEM((E, D, 2 * FC), BF16),
                pltpu.VMEM((E, D, 2 * FC), BF16),
                pltpu.VMEM((E, D, 2 * FC), BF16),
                pltpu.VMEM((NB * T // RG, RG, CC), BF16),
                pltpu.VMEM((4, 2, 2, 2, 2, T, 128), F32),
                pltpu.VMEM((NC, 2, 2, 2, T, 128), F32),
                pltpu.VMEM((NC, 2, 2, T, 128), F32),
                pltpu.VMEM((NC, 2, T, 128), F32),
                pltpu.VMEM((2 * E, T), I32),
                pltpu.SMEM((2 * E, T), I32),
                pltpu.VMEM((E, ndev, 8, T), I32),
                pltpu.VMEM((ndev, E, T), I32),
                dma((4,)),
                dma((ndev - 1,)), dma((ndev - 1,)),
                dma((ndev - 1,)), dma((ndev - 1,)),
                dma((NQ,)), dma((NQ,)), dma((2, NQ)), dma((2, NQ)),
                dma((2, NQ)), dma((2, NQ)), dma((2, NQ)), dma((2, NQ)), dma((2, NQ)), dma((2, NQ)),
                dma((NSLOT, 2)), dma,
                dma((NC,)), dma((NC,)), dma((NC, 2)), dma((NC, 2)), dma((NC, 2)), dma((NC, 2)),
            ],
            compiler_params=pltpu.CompilerParams(
                collective_id=0, has_side_effects=True, vmem_limit_bytes=67043328),
            name='moe_block',
        )(tokens, expert_ids.T, norm_gain, w_router.T, w_gate, w_up, w_down)

    row_spec = P(('dp', 'ep'), None)
    expert_spec = P('ep', None, None)
    return jax.shard_map(device_step, mesh=mesh,
                         in_specs=(row_spec, row_spec, P(None), P(None, None), expert_spec, expert_spec, expert_spec),
                         out_specs=row_spec, check_vma=False)
```

```python
import functools

import jax
import jax.numpy as jnp
from jax import lax
from jax.experimental import pallas as pl
from jax.experimental.pallas import tpu as pltpu
from jax.sharding import PartitionSpec as P

NORM_EPS = 1e-5
MESH = pl.DeviceIdType.MESH
F32, BF16, I32 = jnp.float32, jnp.bfloat16, jnp.int32
FC = 128
CC = 256
NSLOT = 3
NQ = 4
WIN = 256
RG = 16


def moe_kernel(dims, x_hbm, ids_hbm, gain_hbm, wr_hbm, w1_ref, w3_ref, w2_ref, out_ref,
               x_ref, gain_ref, wr_ref, xg, idsg, gsrc, gdst, gbuf, xs, hbuf, gates, wa, wb, wc, obuf, part, rd, rp1, rp2,
               meta_v, meta_s, posrow, posv, s_in,
               s_ids, r_ids, s_gt, r_gt, s_sib, r_sib, s_nb, r_nb, s_dg, r_dg, s_sf, r_sf, s_sd, r_sd, s_w, s_meta,
               d_s, d_r, p1_s, p1_r, p2_s, p2_r):
    T, D, FF, E, NDEV, NB = dims
    NF, NC = FF // FC, D // CC
    HT = T // 2
    me = lax.axis_index('ep')
    core = me % 2
    cx = (me // 2) % 2
    cy = me // 4
    sib = cy * 4 + cx * 2 + (1 - core)
    xn = cy * 4 + (1 - cx) * 2 + core
    yn = (1 - cy) * 4 + cx * 2 + core

    def remote(src, dst, ss, rs, dev):
        return pltpu.make_async_remote_copy(src_ref=src, dst_ref=dst, send_sem=ss, recv_sem=rs,
                                            device_id={'ep': dev}, device_id_type=MESH)

    wslots = (wa, wb, wc)

    def a_copies(f, slot):
        cols = pl.ds(pl.multiple_of(f * FC, FC), FC)
        return (pltpu.make_async_copy(w1_ref.at[:, :, cols], wslots[slot].at[:, :, pl.ds(0, FC)], s_w.at[slot, 0]),
                pltpu.make_async_copy(w3_ref.at[:, :, cols], wslots[slot].at[:, :, pl.ds(FC, FC)], s_w.at[slot, 1]))

    def b_copy(c, slot, half):
        cols = pl.ds(pl.multiple_of(c * CC, CC), CC)
        rows = pl.ds(pl.multiple_of(half * FF, FF), FF)
        return pltpu.make_async_copy(w2_ref.at[:, :, cols], wslots[slot].at[:, rows, :], s_w.at[slot, half])

    barrier = pltpu.get_barrier_semaphore()
    for k in range(1, NDEV):
        pl.semaphore_signal(barrier, inc=1, device_id={'ep': (me + k) % NDEV}, device_id_type=MESH)

    ins = [pltpu.make_async_copy(a, b, s_in.at[k]) for k, (a, b) in enumerate(
        ((x_hbm, x_ref), (gain_hbm, gain_ref), (ids_hbm, idsg.at[me]), (wr_hbm, wr_ref)))]
    for cp in ins:
        cp.start()
    def first_weights(slot):
        for cp in a_copies(slot, slot):
            cp.start()

    own = xg.at[me // 2, core]

    ins[0].wait()
    ins[1].wait()
    gain = gain_ref[...].astype(F32).reshape(1, D)
    for i in range(T // 16):
        rows = pl.ds(i * 16, 16)
        t = x_ref[rows, :].astype(F32)
        inv = lax.rsqrt(jnp.mean(t * t, axis=1, keepdims=True) + NORM_EPS)
        xg[me // 2, core, rows, :] = (t * inv * gain).astype(BF16)
    ins[2].wait()
    pl.semaphore_wait(barrier, NDEV - 1)

    def ids_copy(k):
        return remote(idsg.at[me], idsg.at[me], s_ids.at[k - 1], r_ids.at[k - 1], (me + k) % NDEV)

    def gate_copy(k):
        to = (me + k) % NDEV
        return remote(gsrc.at[to], gdst.at[me], s_gt.at[k - 1], r_gt.at[k - 1], to)

    chip_x = cy * 2 + (1 - cx)
    chip_y = (1 - cy) * 2 + cx
    chip_d = (1 - cy) * 2 + (1 - cx)
    chip_me = cy * 2 + cx
    QC = D // NQ

    def part_of(chip, q, rows=pl.ds(0, T)):
        return xg.at[chip, core, rows, pl.ds(pl.multiple_of(q * QC, QC), QC)]

    def to_sib(q):
        return remote(part_of(chip_me, q), part_of(chip_me, q), s_sib.at[q], r_sib.at[q], sib)

    def to_nb(k, q):
        return remote(part_of(chip_me, q), part_of(chip_me, q), s_nb.at[k, q], r_nb.at[k, q], (xn, yn)[k])

    halves = (pl.ds(0, HT), pl.ds(HT, HT))

    def to_diag(k, q):
        src = part_of((chip_x, chip_y)[k], q, halves[k])
        return remote(src, src, s_dg.at[k, q], r_dg.at[k, q], (yn, xn)[k])

    def nb_sib(k, q):
        src = part_of((chip_x, chip_y)[k], q)
        return remote(src, src, s_sf.at[k, q], r_sf.at[k, q], sib)

    def diag_sib(k, q):
        src = part_of(chip_d, q, halves[k])
        return remote(src, src, s_sd.at[k, q], r_sd.at[k, q], sib)

    for k in range(1, NDEV):
        ids_copy(k).start()
    for q in range(NQ):
        to_nb(0, q).start()
        to_nb(1, q).start()
        to_sib(q).start()

    ins[3].wait()
    logits = lax.dot_general(wr_ref[...], own[...], (((1,), (1,)), ((), ())), preferred_element_type=F32)
    ex = jnp.exp(logits - jnp.max(logits, axis=0, keepdims=True))
    prob = ex / jnp.sum(ex, axis=0, keepdims=True)
    for r in range(NDEV):
        gsrc[r] = prob[r * E:(r + 1) * E]
    gdst[me] = gsrc[me]

    for k in range(1, NDEV):
        ids_copy(k).wait_recv()
    sub_e = lax.broadcasted_iota(I32, (E, T), 0)
    lane = lax.broadcasted_iota(I32, (E, T), 1)
    masks = []
    for s in range(NDEV):
        ids = idsg[s]
        m = jnp.zeros((E, T), I32)
        for j in range(ids.shape[0]):
            m = m + (ids[j:j + 1, :] == sub_e + me * E).astype(I32)
        masks.append(m)
    tri = (lax.broadcasted_iota(I32, (T, T), 0) <= lax.broadcasted_iota(I32, (T, T), 1)).astype(F32).astype(BF16)
    counts = [jnp.sum(m, axis=1, keepdims=True) for m in masks]
    total = counts[0]
    for s in range(1, NDEV):
        total = total + counts[s]
    nblk = (total + (T - 1)) // T
    nblk = jnp.broadcast_to(nblk, (E, T))
    start = jnp.zeros((E, T), I32)
    for e in range(E - 1):
        start = start + jnp.where(sub_e > e, jnp.broadcast_to(nblk[e:e + 1, :], (E, T)), 0)
    eid = jnp.sum((start + nblk <= lane).astype(I32), axis=0, keepdims=True)
    eid = jnp.minimum(eid, E - 1)
    base = start * T
    wst = jnp.zeros((E, T), I32)
    for s in range(NDEV):
        rank = jnp.dot(masks[s].astype(F32).astype(BF16), tri, preferred_element_type=F32).astype(I32)
        pos = jnp.where(masks[s] > 0, base + rank - 1, -1)
        posv[s] = pos
        for e in range(E):
            posrow[e, s] = jnp.broadcast_to(pos[e:e + 1, :], (8, T))
        w0 = jnp.minimum(base // RG, (NB * T - WIN) // RG)
        wst = wst + jnp.where(lane == s, w0, 0)
        base = base + counts[s]
    meta_v[0:E, :] = wst
    meta_v[E:2 * E, :] = jnp.broadcast_to(eid, (E, T))
    meta_copy = pltpu.make_async_copy(meta_v, meta_s, s_meta)
    meta_copy.start()
    meta_copy.wait()
    for k in range(1, NDEV):
        gate_copy(k).start()

    def build(b, carry):
        e = meta_s[E, b]
        rows = lax.broadcasted_iota(I32, (T, T), 0) + b * T
        for s in range(NDEV):
            p = jnp.broadcast_to(posrow[e, s][0:1, :], (T, T))
            gbuf[s // 2, pl.ds(pl.multiple_of(b * T, T), T), (s % 2) * T:(s % 2 + 1) * T] = (p == rows).astype(F32).astype(BF16)
        return carry

    lax.fori_loop(0, NB, build, 0)
    MR = NB * T // 4

    def gather(q, chips, add):
        cols = pl.ds(pl.multiple_of(q * QC, QC), QC)
        for i in range(4):
            rows = pl.ds(i * MR, MR)
            got = None
            for chip in chips:
                one = jnp.dot(gbuf[chip, rows, :], xg[chip, :, :, cols].reshape(2 * T, QC), preferred_element_type=F32)
                got = one if got is None else got + one
            got = got.astype(BF16)
            xs[rows, cols] = xs[rows, cols] + got if add else got

    def forward(q):
        for k in range(2):
            to_nb(k, q).wait_recv()
            to_diag(k, q).start()
            nb_sib(k, q).start()

    def gather_near(q):
        to_sib(q).wait_recv()
        for k in range(2):
            nb_sib(k, q).wait_recv()
        gather(q, (chip_me, chip_x, chip_y), False)

    def forward_diag(q):
        for k in range(2):
            to_diag(k, q).wait_recv()
            diag_sib(k, q).start()

    forward(0)
    first_weights(0)

    def near(q, carry):
        @pl.when(q == 1)
        def _():
            first_weights(1)

        @pl.when(q == NQ - 1)
        def _():
            first_weights(2)

        @pl.when(q < NQ - 1)
        def _():
            forward(q + 1)

        @pl.when(q == NQ - 1)
        def _():
            forward_diag(0)
        gather_near(q)
        return carry

    lax.fori_loop(0, NQ, near, 0)

    def far(q, carry):
        @pl.when(q < NQ - 1)
        def _():
            forward_diag(q + 1)
        for k in range(2):
            diag_sib(k, q).wait_recv()
        gather(q, (chip_d,), True)
        return carry

    lax.fori_loop(0, NQ, far, 0)
    for k in range(1, NDEV):
        gate_copy(k).wait_recv()

    wlane = lax.broadcasted_iota(I32, (T, WIN), 1)

    def window_rows(s, e):
        return pl.ds(pl.multiple_of((s % 2 * E + e) * T, T), T)

    def windows(s):
        padded = jnp.concatenate([posv[s], jnp.zeros((T - E, T), I32)], axis=0).astype(F32)
        col = padded.T
        for e in range(E):
            pc = col[:, e:e + 1].astype(I32)
            gbuf[s // 2, window_rows(s, e), :] = (pc == wlane + meta_s[e, s] * RG).astype(F32).astype(BF16)
        gates[s] = jnp.concatenate([gdst[s], jnp.zeros((T - E, T), F32)], axis=0).T

    def hidden(f, slot):
        for cp in a_copies(f, slot):
            cp.wait()
        windows(f)
        cols = pl.ds(pl.multiple_of(f * FC, FC), FC)
        for b in range(NB):
            e = meta_s[E, b]
            acc = jnp.dot(xs[b * T:(b + 1) * T, :], wslots[slot][e], preferred_element_type=F32)
            hg, hu = acc[:, :FC], acc[:, FC:]
            hbuf[b * T:(b + 1) * T, cols] = (jax.nn.silu(hg) * hu).astype(BF16)

    order = (2, 0)

    def hidden_three(g, carry):
        for slot in range(NSLOT):
            f = g * NSLOT + slot

            @pl.when(f < NF)
            def _():
                hidden(f, slot)

            @pl.when(f < NF - NSLOT)
            def _():
                for cp in a_copies(f + NSLOT, slot):
                    cp.start()

            if slot in order:
                @pl.when((f >= NF - NSLOT) & (f < NF))
                def _():
                    for h in range(2):
                        b_copy(order.index(slot) * 2 + h, slot, h).start()
        return carry

    lax.fori_loop(0, (NF + NSLOT - 1) // NSLOT, hidden_three, 0)

    def d2d(j):
        return remote(part.at[j % 4, 1 - core], rd.at[j], d_s.at[j], d_r.at[j], sib)

    def first_hop(j):
        return (remote(part.at[j % 4, core, 0, :, 1 - cx], rp1.at[j, 0], p1_s.at[j, 0], p1_r.at[j, 0], xn),
                remote(part.at[j % 4, core, 1, 1 - cy], rp1.at[j, 1], p1_s.at[j, 1], p1_r.at[j, 1], yn))

    def second_hop(j):
        return (remote(part.at[j % 4, core, 0, 1 - cy, cx], rp2.at[j, 0], p2_s.at[j, 0], p2_r.at[j, 0], yn),
                remote(part.at[j % 4, core, 1, cy, 1 - cx], rp2.at[j, 1], p2_s.at[j, 1], p2_r.at[j, 1], xn))

    def combine(c, to_core):
        for ch in range(NDEV // 2):
            s = ch * 2 + to_core
            acc = jnp.zeros((T, CC), F32)
            for e in range(E):
                r0 = meta_s[e, s]
                rows = jnp.concatenate([obuf[r0 + k] for k in range(WIN // RG)], axis=0)
                got = jnp.dot(gbuf[s // 2, window_rows(s, e), :], rows, preferred_element_type=F32)
                acc = acc + gates[s, :, e:e + 1] * got
            for h in range(2):
                part[c % 4, to_core, h, ch // 2, ch % 2] = acc[:, h * 128:(h + 1) * 128]

    def outputs(half, slot):
        rows = pl.ds(pl.multiple_of(half * FF, FF), FF)
        for b in range(NB):
            e = meta_s[E, b]
            acc = jnp.dot(hbuf[b * T:(b + 1) * T, :], wslots[slot][e, rows, :], preferred_element_type=F32)
            obuf[b * (T // RG):(b + 1) * (T // RG)] = acc.astype(BF16).reshape(T // RG, RG, CC)

    def stage_one(i):
        @pl.when((i >= 1) & (i < NC + 1))
        def _():
            j = i - 1
            d2d(j).wait_recv()
            for h in range(2):
                for ch in range(NDEV // 2):
                    at = (j % 4, core, h, ch // 2, ch % 2)
                    part[at] = part[at] + rd[j, h, ch // 2, ch % 2]
            for cp in first_hop(j):
                cp.start()

    def stage_two(i):
        @pl.when((i >= 2) & (i < NC + 2))
        def _():
            j = i - 2
            for h, cp in enumerate(first_hop(j)):
                cp.wait_recv()
                for k in range(2):
                    at = (j % 4, core, h, k, cx) if h == 0 else (j % 4, core, h, cy, k)
                    part[at] = part[at] + rp1[j, h, k]
            for cp in second_hop(j):
                cp.start()

        @pl.when(i >= 3)
        def _():
            j = i - 3
            for h, cp in enumerate(second_hop(j)):
                cp.wait_recv()
                cols = pl.ds(pl.multiple_of(j * CC + h * 128, 128), 128)
                moe = part[j % 4, core, h, cy, cx] + rp2[j, h]
                out_ref[:, cols] = (x_ref[:, cols].astype(F32) + moe).astype(BF16)
            d2d(j).wait_send()
            for cp in first_hop(j):
                cp.wait_send()
            for cp in second_hop(j):
                cp.wait_send()

    def four(g, carry):
        for t in range(2):
            slot = order[t]
            for h in range(2):
                b_copy(g * 4 + t * 2 + h, slot, h).wait()

            def two(half, inner):
                i = g * 4 + t * 2 + half
                outputs(half, slot)
                stage_one(i)
                combine(i, 1 - core)
                d2d(i).start()
                combine(i, core)
                stage_two(i)
                return inner
            lax.fori_loop(0, 2, two, 0)

            @pl.when(g < NC // 4 - 1)
            def _():
                for h in range(2):
                    b_copy((g + 1) * 4 + t * 2 + h, slot, h).start()
        return carry

    lax.fori_loop(0, NC // 4, four, 0)

    def last(i, carry):
        stage_one(i)
        stage_two(i)
        return carry

    lax.fori_loop(NC, NC + 3, last, 0)

    for k in range(1, NDEV):
        ids_copy(k).wait_send()
        gate_copy(k).wait_send()
    for q in range(NQ):
        to_sib(q).wait_send()
        for k in range(2):
            for move in (to_nb, to_diag, nb_sib, diag_sib):
                move(k, q).wait_send()


def solution(mesh):
    ndev = mesh.shape['ep']

    def device_step(tokens, expert_ids, norm_gain, w_router, w_gate, w_up, w_down):
        T, D = tokens.shape
        top = expert_ids.shape[1]
        E, _, FF = w_gate.shape
        most = 3 * T * top // 2
        NB = (most + E * (T - 1)) // T
        NC = D // CC
        dims = (T, D, FF, E, ndev, NB)
        vmem = pl.BlockSpec(memory_space=pltpu.VMEM)
        hbm = pl.BlockSpec(memory_space=pl.ANY)
        dma = pltpu.SemaphoreType.DMA
        return pl.pallas_call(
            functools.partial(moe_kernel, dims),
            out_shape=pltpu.VMEM((T, D), BF16),
            in_specs=[hbm] * 7,
            out_specs=vmem,
            scratch_shapes=[
                pltpu.VMEM((T, D), BF16),
                pltpu.VMEM((D,), BF16),
                pltpu.VMEM((ndev * E, D), BF16),
                pltpu.VMEM((ndev // 2, 2, T, D), BF16),
                pltpu.VMEM((ndev, top, T), I32),
                pltpu.VMEM((ndev, E, T), F32),
                pltpu.VMEM((ndev, E, T), F32),
                pltpu.VMEM((ndev // 2, NB * T, 2 * T), BF16),
                pltpu.VMEM((NB * T, D), BF16),
                pltpu.VMEM((NB * T, FF), BF16),
                pltpu.VMEM((ndev, T, 128), F32),
                pltpu.VMEM((E, D, 2 * FC), BF16),
                pltpu.VMEM((E, D, 2 * FC), BF16),
                pltpu.VMEM((E, D, 2 * FC), BF16),
                pltpu.VMEM((NB * T // RG, RG, CC), BF16),
                pltpu.VMEM((4, 2, 2, 2, 2, T, 128), F32),
                pltpu.VMEM((NC, 2, 2, 2, T, 128), F32),
                pltpu.VMEM((NC, 2, 2, T, 128), F32),
                pltpu.VMEM((NC, 2, T, 128), F32),
                pltpu.VMEM((2 * E, T), I32),
                pltpu.SMEM((2 * E, T), I32),
                pltpu.VMEM((E, ndev, 8, T), I32),
                pltpu.VMEM((ndev, E, T), I32),
                dma((4,)),
                dma((ndev - 1,)), dma((ndev - 1,)),
                dma((ndev - 1,)), dma((ndev - 1,)),
                dma((NQ,)), dma((NQ,)), dma((2, NQ)), dma((2, NQ)),
                dma((2, NQ)), dma((2, NQ)), dma((2, NQ)), dma((2, NQ)), dma((2, NQ)), dma((2, NQ)),
                dma((NSLOT, 2)), dma,
                dma((NC,)), dma((NC,)), dma((NC, 2)), dma((NC, 2)), dma((NC, 2)), dma((NC, 2)),
            ],
            compiler_params=pltpu.CompilerParams(
                collective_id=0, has_side_effects=True, vmem_limit_bytes=66300000),
            name='moe_block',
        )(tokens, expert_ids.T, norm_gain, w_router.T, w_gate, w_up, w_down)

    row_spec = P(('dp', 'ep'), None)
    expert_spec = P('ep', None, None)
    return jax.shard_map(device_step, mesh=mesh,
                         in_specs=(row_spec, row_spec, P(None), P(None, None), expert_spec, expert_spec, expert_spec),
                         out_specs=row_spec, check_vma=False)
```

```python
import functools

import jax
import jax.numpy as jnp
from jax import lax
from jax.experimental import pallas as pl
from jax.experimental.pallas import tpu as pltpu
from jax.sharding import PartitionSpec as P

NORM_EPS = 1e-5
MESH = pl.DeviceIdType.MESH
F32, BF16, I32 = jnp.float32, jnp.bfloat16, jnp.int32
FC = 128
CC = 256
NSLOT = 3
NQ = 4
WIN = 256
RG = 16


def moe_kernel(dims, x_hbm, ids_hbm, gain_hbm, wr_hbm, w1_ref, w3_ref, w2_ref, out_ref,
               x_ref, gain_ref, wr_ref, xg, idsg, gsrc, gdst, gbuf, xs, hbuf, gates, wa, wb, wc, obuf, part, rd, rp1, rp2,
               meta_v, meta_s, posrow, posv, s_in,
               s_ids, r_ids, s_gt, r_gt, s_sib, r_sib, s_nb, r_nb, s_dg, r_dg, s_sf, r_sf, s_sd, r_sd, s_w, s_meta,
               d_s, d_r, p1_s, p1_r, p2_s, p2_r):
    T, D, FF, E, NDEV, NB = dims
    NF, NC = FF // FC, D // CC
    HT = T // 2
    me = lax.axis_index('ep')
    core = me % 2
    cx = (me // 2) % 2
    cy = me // 4
    sib = cy * 4 + cx * 2 + (1 - core)
    xn = cy * 4 + (1 - cx) * 2 + core
    yn = (1 - cy) * 4 + cx * 2 + core

    def remote(src, dst, ss, rs, dev):
        return pltpu.make_async_remote_copy(src_ref=src, dst_ref=dst, send_sem=ss, recv_sem=rs,
                                            device_id={'ep': dev}, device_id_type=MESH)

    wslots = (wa, wb, wc)

    def a_copies(f, slot):
        cols = pl.ds(pl.multiple_of(f * FC, FC), FC)
        return (pltpu.make_async_copy(w1_ref.at[:, :, cols], wslots[slot].at[:, :, pl.ds(0, FC)], s_w.at[slot, 0]),
                pltpu.make_async_copy(w3_ref.at[:, :, cols], wslots[slot].at[:, :, pl.ds(FC, FC)], s_w.at[slot, 1]))

    def b_copy(c, slot, half):
        cols = pl.ds(pl.multiple_of(c * CC, CC), CC)
        rows = pl.ds(pl.multiple_of(half * FF, FF), FF)
        return pltpu.make_async_copy(w2_ref.at[:, :, cols], wslots[slot].at[:, rows, :], s_w.at[slot, half])

    barrier = pltpu.get_barrier_semaphore()
    for k in range(1, NDEV):
        pl.semaphore_signal(barrier, inc=1, device_id={'ep': (me + k) % NDEV}, device_id_type=MESH)

    ins = [pltpu.make_async_copy(a, b, s_in.at[k]) for k, (a, b) in enumerate(
        ((x_hbm, x_ref), (gain_hbm, gain_ref), (ids_hbm, idsg.at[me]), (wr_hbm, wr_ref)))]
    for cp in ins:
        cp.start()
    def first_weights(slot):
        for cp in a_copies(slot, slot):
            cp.start()

    own = xg.at[me // 2, core]

    ins[0].wait()
    ins[1].wait()
    gain = gain_ref[...].astype(F32).reshape(1, D)
    for i in range(T // 16):
        rows = pl.ds(i * 16, 16)
        t = x_ref[rows, :].astype(F32)
        inv = lax.rsqrt(jnp.mean(t * t, axis=1, keepdims=True) + NORM_EPS)
        xg[me // 2, core, rows, :] = (t * inv * gain).astype(BF16)
    ins[2].wait()
    pl.semaphore_wait(barrier, NDEV - 1)

    def ids_copy(k):
        return remote(idsg.at[me], idsg.at[me], s_ids.at[k - 1], r_ids.at[k - 1], (me + k) % NDEV)

    def gate_copy(k):
        to = (me + k) % NDEV
        return remote(gsrc.at[to], gdst.at[me], s_gt.at[k - 1], r_gt.at[k - 1], to)

    chip_x = cy * 2 + (1 - cx)
    chip_y = (1 - cy) * 2 + cx
    chip_d = (1 - cy) * 2 + (1 - cx)
    chip_me = cy * 2 + cx
    QC = D // NQ

    def part_of(chip, q, rows=pl.ds(0, T)):
        return xg.at[chip, core, rows, pl.ds(pl.multiple_of(q * QC, QC), QC)]

    def to_sib(q):
        return remote(part_of(chip_me, q), part_of(chip_me, q), s_sib.at[q], r_sib.at[q], sib)

    def to_nb(k, q):
        return remote(part_of(chip_me, q), part_of(chip_me, q), s_nb.at[k, q], r_nb.at[k, q], (xn, yn)[k])

    halves = (pl.ds(0, HT), pl.ds(HT, HT))

    def to_diag(k, q):
        src = part_of((chip_x, chip_y)[k], q, halves[k])
        return remote(src, src, s_dg.at[k, q], r_dg.at[k, q], (yn, xn)[k])

    def nb_sib(k, q):
        src = part_of((chip_x, chip_y)[k], q)
        return remote(src, src, s_sf.at[k, q], r_sf.at[k, q], sib)

    def diag_sib(k, q):
        src = part_of(chip_d, q, halves[k])
        return remote(src, src, s_sd.at[k, q], r_sd.at[k, q], sib)

    for k in range(1, NDEV):
        ids_copy(k).start()
    for q in range(NQ):
        to_nb(0, q).start()
        to_nb(1, q).start()
        to_sib(q).start()

    ins[3].wait()
    logits = lax.dot_general(wr_ref[...], own[...], (((1,), (1,)), ((), ())), preferred_element_type=F32)
    ex = jnp.exp(logits - jnp.max(logits, axis=0, keepdims=True))
    prob = ex / jnp.sum(ex, axis=0, keepdims=True)
    for r in range(NDEV):
        gsrc[r] = prob[r * E:(r + 1) * E]
    gdst[me] = gsrc[me]

    for k in range(1, NDEV):
        ids_copy(k).wait_recv()
    sub_e = lax.broadcasted_iota(I32, (E, T), 0)
    lane = lax.broadcasted_iota(I32, (E, T), 1)
    masks = []
    for s in range(NDEV):
        ids = idsg[s]
        m = jnp.zeros((E, T), I32)
        for j in range(ids.shape[0]):
            m = m + (ids[j:j + 1, :] == sub_e + me * E).astype(I32)
        masks.append(m)
    tri = (lax.broadcasted_iota(I32, (T, T), 0) <= lax.broadcasted_iota(I32, (T, T), 1)).astype(F32).astype(BF16)
    counts = [jnp.sum(m, axis=1, keepdims=True) for m in masks]
    total = counts[0]
    for s in range(1, NDEV):
        total = total + counts[s]
    nblk = (total + (T - 1)) // T
    nblk = jnp.broadcast_to(nblk, (E, T))
    start = jnp.zeros((E, T), I32)
    for e in range(E - 1):
        start = start + jnp.where(sub_e > e, jnp.broadcast_to(nblk[e:e + 1, :], (E, T)), 0)
    eid = jnp.sum((start + nblk <= lane).astype(I32), axis=0, keepdims=True)
    eid = jnp.minimum(eid, E - 1)
    base = start * T
    wst = jnp.zeros((E, T), I32)
    for s in range(NDEV):
        rank = jnp.dot(masks[s].astype(F32).astype(BF16), tri, preferred_element_type=F32).astype(I32)
        pos = jnp.where(masks[s] > 0, base + rank - 1, -1)
        posv[s] = pos
        for e in range(E):
            posrow[e, s] = jnp.broadcast_to(pos[e:e + 1, :], (8, T))
        w0 = jnp.minimum(base // RG, (NB * T - WIN) // RG)
        wst = wst + jnp.where(lane == s, w0, 0)
        base = base + counts[s]
    meta_v[0:E, :] = wst
    meta_v[E:2 * E, :] = jnp.broadcast_to(eid, (E, T))
    meta_copy = pltpu.make_async_copy(meta_v, meta_s, s_meta)
    meta_copy.start()
    meta_copy.wait()
    for k in range(1, NDEV):
        gate_copy(k).start()

    def build(b, carry):
        e = meta_s[E, b]
        rows = lax.broadcasted_iota(I32, (T, T), 0) + b * T
        for s in range(NDEV):
            p = jnp.broadcast_to(posrow[e, s][0:1, :], (T, T))
            gbuf[s // 2, pl.ds(pl.multiple_of(b * T, T), T), (s % 2) * T:(s % 2 + 1) * T] = (p == rows).astype(F32).astype(BF16)
        return carry

    lax.fori_loop(0, NB, build, 0)
    MR = NB * T // 4

    def gather(q, chips, add):
        cols = pl.ds(pl.multiple_of(q * QC, QC), QC)
        for i in range(4):
            rows = pl.ds(i * MR, MR)
            got = None
            for chip in chips:
                one = jnp.dot(gbuf[chip, rows, :], xg[chip, :, :, cols].reshape(2 * T, QC), preferred_element_type=F32)
                got = one if got is None else got + one
            got = got.astype(BF16)
            xs[rows, cols] = xs[rows, cols] + got if add else got

    def forward(q):
        for k in range(2):
            to_nb(k, q).wait_recv()
            to_diag(k, q).start()
            nb_sib(k, q).start()

    def gather_near(q):
        to_sib(q).wait_recv()
        for k in range(2):
            nb_sib(k, q).wait_recv()
        gather(q, (chip_me, chip_x, chip_y), False)

    def forward_diag(q):
        for k in range(2):
            to_diag(k, q).wait_recv()
            diag_sib(k, q).start()

    forward(0)
    first_weights(0)

    def near(q, carry):
        @pl.when(q == 1)
        def _():
            first_weights(1)

        @pl.when(q == NQ - 1)
        def _():
            first_weights(2)

        @pl.when(q < NQ - 1)
        def _():
            forward(q + 1)

        @pl.when(q == NQ - 1)
        def _():
            forward_diag(0)
        gather_near(q)
        return carry

    lax.fori_loop(0, NQ, near, 0)

    def far(q, carry):
        @pl.when(q < NQ - 1)
        def _():
            forward_diag(q + 1)
        for k in range(2):
            diag_sib(k, q).wait_recv()
        gather(q, (chip_d,), True)
        return carry

    lax.fori_loop(0, NQ, far, 0)
    for k in range(1, NDEV):
        gate_copy(k).wait_recv()

    wlane = lax.broadcasted_iota(I32, (T, WIN), 1)

    def window_rows(s, e):
        return pl.ds(pl.multiple_of((s % 2 * E + e) * T, T), T)

    def windows(s):
        padded = jnp.concatenate([posv[s], jnp.zeros((T - E, T), I32)], axis=0).astype(F32)
        col = padded.T
        for e in range(E):
            pc = col[:, e:e + 1].astype(I32)
            gbuf[s // 2, window_rows(s, e), :] = (pc == wlane + meta_s[e, s] * RG).astype(F32).astype(BF16)
        gates[s] = jnp.concatenate([gdst[s], jnp.zeros((T - E, T), F32)], axis=0).T

    def hidden(f, slot):
        for cp in a_copies(f, slot):
            cp.wait()
        windows(f)
        cols = pl.ds(pl.multiple_of(f * FC, FC), FC)
        for b in range(NB):
            e = meta_s[E, b]
            acc = jnp.dot(xs[b * T:(b + 1) * T, :], wslots[slot][e], preferred_element_type=F32)
            hg, hu = acc[:, :FC], acc[:, FC:]
            hbuf[b * T:(b + 1) * T, cols] = (jax.nn.silu(hg) * hu).astype(BF16)

    order = (2, 0)

    def hidden_three(g, carry):
        for slot in range(NSLOT):
            f = g * NSLOT + slot

            @pl.when(f < NF)
            def _():
                hidden(f, slot)

            @pl.when(f < NF - NSLOT)
            def _():
                for cp in a_copies(f + NSLOT, slot):
                    cp.start()

            if slot in order:
                @pl.when((f >= NF - NSLOT) & (f < NF))
                def _():
                    for h in range(2):
                        b_copy(order.index(slot) * 2 + h, slot, h).start()
        return carry

    lax.fori_loop(0, (NF + NSLOT - 1) // NSLOT, hidden_three, 0)

    def d2d(j):
        return remote(part.at[j % 4, 1 - core], rd.at[j], d_s.at[j], d_r.at[j], sib)

    def first_hop(j):
        return (remote(part.at[j % 4, core, 0, :, 1 - cx], rp1.at[j, 0], p1_s.at[j, 0], p1_r.at[j, 0], xn),
                remote(part.at[j % 4, core, 1, 1 - cy], rp1.at[j, 1], p1_s.at[j, 1], p1_r.at[j, 1], yn))

    def second_hop(j):
        return (remote(part.at[j % 4, core, 0, 1 - cy, cx], rp2.at[j, 0], p2_s.at[j, 0], p2_r.at[j, 0], yn),
                remote(part.at[j % 4, core, 1, cy, 1 - cx], rp2.at[j, 1], p2_s.at[j, 1], p2_r.at[j, 1], xn))

    def combine(c, to_core):
        for ch in range(NDEV // 2):
            s = ch * 2 + to_core
            acc = jnp.zeros((T, CC), F32)
            for e in range(E):
                r0 = meta_s[e, s]
                rows = jnp.concatenate([obuf[r0 + k] for k in range(WIN // RG)], axis=0)
                got = jnp.dot(gbuf[s // 2, window_rows(s, e), :], rows, preferred_element_type=F32)
                acc = acc + gates[s, :, e:e + 1] * got
            for h in range(2):
                part[c % 4, to_core, h, ch // 2, ch % 2] = acc[:, h * 128:(h + 1) * 128]

    def outputs(half, slot):
        rows = pl.ds(pl.multiple_of(half * FF, FF), FF)
        for b in range(NB):
            e = meta_s[E, b]
            acc = jnp.dot(hbuf[b * T:(b + 1) * T, :], wslots[slot][e, rows, :], preferred_element_type=F32)
            obuf[b * (T // RG):(b + 1) * (T // RG)] = acc.astype(BF16).reshape(T // RG, RG, CC)

    def stage_one(i):
        @pl.when((i >= 1) & (i < NC + 1))
        def _():
            j = i - 1
            d2d(j).wait_recv()
            for h in range(2):
                for ch in range(NDEV // 2):
                    at = (j % 4, core, h, ch // 2, ch % 2)
                    part[at] = part[at] + rd[j, h, ch // 2, ch % 2]
            for cp in first_hop(j):
                cp.start()

    def stage_two(i):
        @pl.when((i >= 2) & (i < NC + 2))
        def _():
            j = i - 2
            for h, cp in enumerate(first_hop(j)):
                cp.wait_recv()
                for k in range(2):
                    at = (j % 4, core, h, k, cx) if h == 0 else (j % 4, core, h, cy, k)
                    part[at] = part[at] + rp1[j, h, k]
            for cp in second_hop(j):
                cp.start()

        @pl.when(i >= 3)
        def _():
            j = i - 3
            for h, cp in enumerate(second_hop(j)):
                cp.wait_recv()
                cols = pl.ds(pl.multiple_of(j * CC + h * 128, 128), 128)
                moe = part[j % 4, core, h, cy, cx] + rp2[j, h]
                out_ref[:, cols] = (x_ref[:, cols].astype(F32) + moe).astype(BF16)
            d2d(j).wait_send()
            for cp in first_hop(j):
                cp.wait_send()
            for cp in second_hop(j):
                cp.wait_send()

    def four(g, carry):
        for t in range(2):
            slot = order[t]
            for h in range(2):
                b_copy(g * 4 + t * 2 + h, slot, h).wait()

            def two(half, inner):
                i = g * 4 + t * 2 + half
                outputs(half, slot)
                stage_one(i)
                combine(i, 1 - core)
                d2d(i).start()
                stage_two(i)
                combine(i, core)
                return inner
            lax.fori_loop(0, 2, two, 0)

            @pl.when(g < NC // 4 - 1)
            def _():
                for h in range(2):
                    b_copy((g + 1) * 4 + t * 2 + h, slot, h).start()
        return carry

    lax.fori_loop(0, NC // 4, four, 0)

    def last(i, carry):
        stage_one(i)
        stage_two(i)
        return carry

    lax.fori_loop(NC, NC + 3, last, 0)

    for k in range(1, NDEV):
        ids_copy(k).wait_send()
        gate_copy(k).wait_send()
    for q in range(NQ):
        to_sib(q).wait_send()
        for k in range(2):
            for move in (to_nb, to_diag, nb_sib, diag_sib):
                move(k, q).wait_send()


def solution(mesh):
    ndev = mesh.shape['ep']

    def device_step(tokens, expert_ids, norm_gain, w_router, w_gate, w_up, w_down):
        T, D = tokens.shape
        top = expert_ids.shape[1]
        E, _, FF = w_gate.shape
        most = 3 * T * top // 2
        NB = (most + E * (T - 1)) // T
        NC = D // CC
        dims = (T, D, FF, E, ndev, NB)
        vmem = pl.BlockSpec(memory_space=pltpu.VMEM)
        hbm = pl.BlockSpec(memory_space=pl.ANY)
        dma = pltpu.SemaphoreType.DMA
        return pl.pallas_call(
            functools.partial(moe_kernel, dims),
            out_shape=pltpu.VMEM((T, D), BF16),
            in_specs=[hbm] * 7,
            out_specs=vmem,
            scratch_shapes=[
                pltpu.VMEM((T, D), BF16),
                pltpu.VMEM((D,), BF16),
                pltpu.VMEM((ndev * E, D), BF16),
                pltpu.VMEM((ndev // 2, 2, T, D), BF16),
                pltpu.VMEM((ndev, top, T), I32),
                pltpu.VMEM((ndev, E, T), F32),
                pltpu.VMEM((ndev, E, T), F32),
                pltpu.VMEM((ndev // 2, NB * T, 2 * T), BF16),
                pltpu.VMEM((NB * T, D), BF16),
                pltpu.VMEM((NB * T, FF), BF16),
                pltpu.VMEM((ndev, T, 128), F32),
                pltpu.VMEM((E, D, 2 * FC), BF16),
                pltpu.VMEM((E, D, 2 * FC), BF16),
                pltpu.VMEM((E, D, 2 * FC), BF16),
                pltpu.VMEM((NB * T // RG, RG, CC), BF16),
                pltpu.VMEM((4, 2, 2, 2, 2, T, 128), F32),
                pltpu.VMEM((NC, 2, 2, 2, T, 128), F32),
                pltpu.VMEM((NC, 2, 2, T, 128), F32),
                pltpu.VMEM((NC, 2, T, 128), F32),
                pltpu.VMEM((2 * E, T), I32),
                pltpu.SMEM((2 * E, T), I32),
                pltpu.VMEM((E, ndev, 8, T), I32),
                pltpu.VMEM((ndev, E, T), I32),
                dma((4,)),
                dma((ndev - 1,)), dma((ndev - 1,)),
                dma((ndev - 1,)), dma((ndev - 1,)),
                dma((NQ,)), dma((NQ,)), dma((2, NQ)), dma((2, NQ)),
                dma((2, NQ)), dma((2, NQ)), dma((2, NQ)), dma((2, NQ)), dma((2, NQ)), dma((2, NQ)),
                dma((NSLOT, 2)), dma,
                dma((NC,)), dma((NC,)), dma((NC, 2)), dma((NC, 2)), dma((NC, 2)), dma((NC, 2)),
            ],
            compiler_params=pltpu.CompilerParams(
                collective_id=0, has_side_effects=True, vmem_limit_bytes=66300000),
            name='moe_block',
        )(tokens, expert_ids.T, norm_gain, w_router.T, w_gate, w_up, w_down)

    row_spec = P(('dp', 'ep'), None)
    expert_spec = P('ep', None, None)
    return jax.shard_map(device_step, mesh=mesh,
                         in_specs=(row_spec, row_spec, P(None), P(None, None), expert_spec, expert_spec, expert_spec),
                         out_specs=row_spec, check_vma=False)
```
